32 devices in a mesh: dp: 2 (over x), tp: 4 (over z), sp: 4 (over y, core).
Axes of the slice: x: 2, y: 2, z: 4, core: 2. Of those that a mesh axis runs over, the one named last changes fastest.
Arguments:
- hidden: bfloat16 [64, 4096], P('dp'), parts along dimension 0
- positions: int32 [64], P('dp'), parts along dimension 0
- k_cache: bfloat16 [64, 32, 512, 128], P('dp', 'tp', 'sp'), parts along dimension 0
- v_cache: bfloat16 [64, 32, 512, 128], P('dp', 'tp', 'sp'), parts along dimension 0
- ln1_gain: bfloat16 [4096], replicated
- ln1_bias: bfloat16 [4096], replicated
- w_query: bfloat16 [4096, 4096], P(None, 'tp')
- b_query: bfloat16 [4096], P('tp')
- w_key: bfloat16 [4096, 4096], P(None, 'tp')
- b_key: bfloat16 [4096], P('tp')
- w_value: bfloat16 [4096, 4096], P(None, 'tp')
- b_value: bfloat16 [4096], P('tp')
- w_out: bfloat16 [4096, 4096], P('tp')
- b_out: bfloat16 [4096], replicated
- ln2_gain: bfloat16 [4096], replicated
- ln2_bias: bfloat16 [4096], replicated
- w_fc1: bfloat16 [4096, 16384], P(None, 'tp')
- b_fc1: bfloat16 [16384], P('tp')
- w_fc2: bfloat16 [16384, 4096], P('tp')
- b_fc2: bfloat16 [4096], replicated
Outputs:
- output 1: bfloat16 [64, 4096], P('dp'), parts along dimension 0
- output 2: bfloat16 [64, 32, 512, 128], P('dp', 'tp', 'sp'), parts along dimension 0
- output 3: bfloat16 [64, 32, 512, 128], P('dp', 'tp', 'sp'), parts along dimension 0
There are 2 independent parts. The reference program is written for one: setup_inputs(seed, part) draws one part's arguments, and reference() takes and returns one part's arrays. A program takes and returns all parts, laid end to end along the dimension named above; an argument that names none is the same for every part.
All inputs are finite; a program needn't handle non-finite values.
Results may differ from the reference program's by a relative error of at most 0.0078411.
Values sent between devices are 32-bit elements.
A program may use at most 1 GiB of HBM per device.

```python
import jax
import jax.numpy as jnp
from jax import lax

MODEL_DIM = 4096
FF_DIM = 16384
NUM_HEADS = 32
HEAD_DIM = 128
BATCH_SEQS = 32
CACHE_LEN = 512
LN_EPS = 1e-5


def draw_normal(rng_key, out_shape, spread):
    return jax.random.normal(rng_key, out_shape, jnp.float32) * spread


def setup_inputs(seed: int = 0, part: int = 0) -> dict:
    base_key = jax.random.key(seed)
    shared_keys = jax.random.split(base_key, 16)
    part_keys = jax.random.split(jax.random.fold_in(base_key, part), 8)
    in_scale = MODEL_DIM ** -0.5
    ff_scale = FF_DIM ** -0.5
    pos_ramp = (2.0 * jnp.arange(CACHE_LEN, dtype=jnp.float32) / (CACHE_LEN - 1) - 1.0)[None, None, :, None]
    cache_shape = (BATCH_SEQS, NUM_HEADS, CACHE_LEN, HEAD_DIM)
    drift_shape = (BATCH_SEQS, NUM_HEADS, 1, HEAD_DIM)
    k_cache = draw_normal(part_keys[0], cache_shape, 1.0) + pos_ramp * draw_normal(part_keys[1], drift_shape, 1.5)
    v_cache = (draw_normal(part_keys[2], cache_shape, 1.0) + draw_normal(part_keys[3], drift_shape, 1.0)
               + pos_ramp * draw_normal(part_keys[4], drift_shape, 1.5))
    start_pos = jax.random.randint(part_keys[5], (BATCH_SEQS,), 0, CACHE_LEN)
    full_row = jax.random.randint(part_keys[6], (), 0, BATCH_SEQS)
    positions = jnp.where(jnp.arange(BATCH_SEQS) == full_row, CACHE_LEN - 1, start_pos).astype(jnp.int32)
    return {
        'hidden': draw_normal(part_keys[7], (BATCH_SEQS, MODEL_DIM), 1.0).astype(jnp.bfloat16),
        'positions': positions,
        'k_cache': k_cache.astype(jnp.bfloat16),
        'v_cache': v_cache.astype(jnp.bfloat16),
        'ln1_gain': (1.0 + draw_normal(shared_keys[0], (MODEL_DIM,), 0.3)).astype(jnp.bfloat16),
        'ln1_bias': draw_normal(shared_keys[1], (MODEL_DIM,), 0.3).astype(jnp.bfloat16),
        'w_query': draw_normal(shared_keys[2], (MODEL_DIM, MODEL_DIM), in_scale).astype(jnp.bfloat16),
        'b_query': draw_normal(shared_keys[3], (MODEL_DIM,), 0.5).astype(jnp.bfloat16),
        'w_key': draw_normal(shared_keys[4], (MODEL_DIM, MODEL_DIM), in_scale).astype(jnp.bfloat16),
        'b_key': draw_normal(shared_keys[5], (MODEL_DIM,), 0.5).astype(jnp.bfloat16),
        'w_value': draw_normal(shared_keys[6], (MODEL_DIM, MODEL_DIM), in_scale).astype(jnp.bfloat16),
        'b_value': draw_normal(shared_keys[7], (MODEL_DIM,), 0.5).astype(jnp.bfloat16),
        'w_out': draw_normal(shared_keys[8], (MODEL_DIM, MODEL_DIM), in_scale).astype(jnp.bfloat16),
        'b_out': draw_normal(shared_keys[9], (MODEL_DIM,), 0.5).astype(jnp.bfloat16),
        'ln2_gain': (1.0 + draw_normal(shared_keys[10], (MODEL_DIM,), 0.3)).astype(jnp.bfloat16),
        'ln2_bias': draw_normal(shared_keys[11], (MODEL_DIM,), 0.3).astype(jnp.bfloat16),
        'w_fc1': draw_normal(shared_keys[12], (MODEL_DIM, FF_DIM), in_scale).astype(jnp.bfloat16),
        'b_fc1': draw_normal(shared_keys[13], (FF_DIM,), 0.5).astype(jnp.bfloat16),
        'w_fc2': draw_normal(shared_keys[14], (FF_DIM, MODEL_DIM), ff_scale).astype(jnp.bfloat16),
        'b_fc2': draw_normal(shared_keys[15], (MODEL_DIM,), 0.5).astype(jnp.bfloat16),
    }


def layer_norm(values, ln_gain, ln_bias):
    as_f32 = values.astype(jnp.float32)
    centered = as_f32 - as_f32.mean(-1, keepdims=True)
    variance = (centered * centered).mean(-1, keepdims=True)
    return (centered * lax.rsqrt(variance + LN_EPS) * ln_gain.astype(jnp.float32) + ln_bias.astype(jnp.float32)).astype(jnp.bfloat16)


def project(normed, weight, bias_vec):
    return jnp.dot(normed, weight, preferred_element_type=jnp.float32) + bias_vec.astype(jnp.float32)


def attend_one(operands):
    query_row, k_row, v_row, pos_row = operands
    scores = jnp.einsum('hd,hsd->hs', query_row.astype(jnp.float32), k_row.astype(jnp.float32))
    valid_mask = jnp.arange(CACHE_LEN)[None, :] <= pos_row
    scores = jnp.where(valid_mask, scores, -1e30)
    weights = jnp.where(valid_mask, jnp.exp(scores - scores.max(-1, keepdims=True)), 0.0)
    mixed_out = jnp.einsum('hs,hsd->hd', weights, v_row.astype(jnp.float32))
    return mixed_out / weights.sum(-1)[:, None]


def reference(hidden, positions, k_cache, v_cache, ln1_gain, ln1_bias, w_query, b_query, w_key, b_key, w_value, b_value, w_out, b_out, ln2_gain, ln2_bias, w_fc1, b_fc1, w_fc2, b_fc2):
    head_shape = (BATCH_SEQS, NUM_HEADS, HEAD_DIM)
    normed = layer_norm(hidden, ln1_gain, ln1_bias)
    query_vec = (project(normed, w_query, b_query) * HEAD_DIM ** -0.5).astype(jnp.bfloat16).reshape(head_shape)
    new_key = project(normed, w_key, b_key).astype(jnp.bfloat16).reshape(head_shape)
    new_value = project(normed, w_value, b_value).astype(jnp.bfloat16).reshape(head_shape)
    at_slot = (jnp.arange(CACHE_LEN)[None, :] == positions[:, None])[:, None, :, None]
    k_next = jnp.where(at_slot, new_key[:, :, None, :], k_cache)
    v_next = jnp.where(at_slot, new_value[:, :, None, :], v_cache)
    mixed_out = lax.map(attend_one, (query_vec, k_next, v_next, positions))
    attn_vec = mixed_out.astype(jnp.bfloat16).reshape(BATCH_SEQS, MODEL_DIM)
    attn_sum = jnp.dot(attn_vec, w_out, preferred_element_type=jnp.float32)
    resid_one = (hidden.astype(jnp.float32) + attn_sum + b_out.astype(jnp.float32)).astype(jnp.bfloat16)
    normed_two = layer_norm(resid_one, ln2_gain, ln2_bias)
    activated = jax.nn.relu(project(normed_two, w_fc1, b_fc1)).astype(jnp.bfloat16)
    mlp_sum = jnp.dot(activated, w_fc2, preferred_element_type=jnp.float32)
    result = (resid_one.astype(jnp.float32) + mlp_sum + b_fc2.astype(jnp.float32)).astype(jnp.bfloat16)
    return result, k_next, v_next
```

```python
import jax
import jax.numpy as jnp
from jax import lax
from jax.experimental import pallas as pl
from jax.experimental.pallas import tpu as pltpu
from jax.sharding import PartitionSpec as P

LN_EPS = 1e-5
NEG = -1e30
F32 = jnp.float32
BF16 = jnp.bfloat16
MESH = pl.DeviceIdType.MESH
ROWS = 32
HALF_ROWS = 16
DIM = 4096
HEADS = 8
HEAD_DIM = 128
BLOCK_LEN = 128
MIB = 1 << 20


def any_spec():
    return pl.BlockSpec(memory_space=pltpu.HBM)


def vmem_spec():
    return pl.BlockSpec(memory_space=pltpu.VMEM)


def remote(src, dst, send_sem, recv_sem, device):
    return pltpu.make_async_remote_copy(src_ref=src, dst_ref=dst, send_sem=send_sem, recv_sem=recv_sem,
                                        device_id=device, device_id_type=MESH)


def dyn(start, size):
    return pl.ds(pl.multiple_of(start, size), size)


QKV_CHUNKS = 4
QKV_ROWS = DIM // QKV_CHUNKS


def as_row(vec_ref):
    return vec_ref[...].astype(F32)[None, :]


def qkv_kernel(h_hbm, g_hbm, b_hbm, wq_ref, wk_ref, wv_ref, bq_hbm, bk_hbm, bv_hbm, out_ref,
               h_buf, g_buf, b_buf, bq_buf, bk_buf, bv_buf, bias_rows, wbuf, norm, send, recv, vsem, wsem, ssem, rsem):
    smalls = [pltpu.make_async_copy(src, dst, vsem.at[n]) for n, (src, dst) in enumerate((
        (h_hbm, h_buf), (g_hbm, g_buf), (b_hbm, b_buf), (bq_hbm, bq_buf), (bk_hbm, bk_buf), (bv_hbm, bv_buf)))]
    for copy in smalls:
        copy.start()
    sp = lax.axis_index('sp')
    core = lax.rem(sp, 2)
    partner = sp + 1 - 2 * core
    cols = dyn(core * 512, 512)
    copies = []
    for i, weight in enumerate((wq_ref, wk_ref, wv_ref)):
        for j in range(QKV_CHUNKS):
            rows = pl.ds(j * QKV_ROWS, QKV_ROWS)
            copy = pltpu.make_async_copy(weight.at[rows, cols], wbuf.at[i, rows, :], wsem.at[i, j])
            copy.start()
            copies.append(copy)
    barrier = pltpu.get_barrier_semaphore()
    pl.semaphore_signal(barrier, inc=1, device_id={'sp': partner}, device_id_type=MESH)

    for copy in smalls:
        copy.wait()
    values = h_buf[...].astype(F32)
    centered = values - jnp.mean(values, -1, keepdims=True)
    variance = jnp.mean(centered * centered, -1, keepdims=True)
    norm[...] = (centered * lax.rsqrt(variance + LN_EPS) * as_row(g_buf) + as_row(b_buf)).astype(BF16)
    for i, buf in enumerate((bq_buf, bk_buf, bv_buf)):
        bias_rows[i] = as_row(buf)

    pl.semaphore_wait(barrier, 1)
    sends = []
    for i in range(3):
        total = None
        for j in range(QKV_CHUNKS):
            copies[i * QKV_CHUNKS + j].wait()
            rows = pl.ds(j * QKV_ROWS, QKV_ROWS)
            part = jnp.dot(norm[:, rows], wbuf[i, rows, :], preferred_element_type=F32)
            total = part if total is None else total + part
        total = total + bias_rows[i, :, cols]
        if i == 0:
            total = total * HEAD_DIM ** -0.5
        total = total.astype(BF16).astype(F32)
        for h in range(4):
            send[i, h] = total[:, h * 128:(h + 1) * 128]
        copy = remote(send.at[i], recv.at[i], ssem.at[i], rsem.at[i], {'sp': partner})
        copy.start()
        sends.append(copy)
        for h in range(4):
            out_ref[i, core * 4 + h] = total[:, h * 128:(h + 1) * 128]
    for i in range(3):
        sends[i].wait_recv()
        for h in range(4):
            out_ref[i, (1 - core) * 4 + h] = recv[i, h]
    for i in range(3):
        sends[i].wait_send()


def qkv_call(hidden, gain, bias, w_query, b_query, w_key, b_key, w_value, b_value):
    return pl.pallas_call(
        qkv_kernel,
        out_shape=jax.ShapeDtypeStruct((3, HEADS, ROWS, HEAD_DIM), F32),
        in_specs=[any_spec()] * 9,
        out_specs=vmem_spec(),
        scratch_shapes=[
            pltpu.VMEM((ROWS, DIM), BF16),
            pltpu.VMEM((DIM,), BF16), pltpu.VMEM((DIM,), BF16),
            pltpu.VMEM((1024,), BF16), pltpu.VMEM((1024,), BF16), pltpu.VMEM((1024,), BF16),
            pltpu.VMEM((3, 1, 1024), F32),
            pltpu.VMEM((3, DIM, 512), BF16),
            pltpu.VMEM((ROWS, DIM), BF16),
            pltpu.VMEM((3, 4, ROWS, 128), F32),
            pltpu.VMEM((3, 4, ROWS, 128), F32),
            pltpu.SemaphoreType.DMA((6,)),
            pltpu.SemaphoreType.DMA((3, QKV_CHUNKS)),
            pltpu.SemaphoreType.DMA((3,)),
            pltpu.SemaphoreType.DMA((3,)),
        ],
        compiler_params=pltpu.CompilerParams(collective_id=0, has_side_effects=True, vmem_limit_bytes=24 * MIB),
        name='qkv',
    )(hidden, gain, bias, w_query, w_key, w_value, b_query, b_key, b_value)


CHUNK = 4
NUM_CHUNKS = ROWS // CHUNK


def attn_kernel(pos_ref, qkv_ref, k_hbm, v_hbm, k_out, v_out, o_ref, st_ref, kbuf, vbuf, qs, kin, vin, kdone, vdone):
    base = lax.axis_index('sp') * BLOCK_LEN

    def chunk_copy(src, dst, sem, p):
        rows = pl.ds(p * CHUNK, CHUNK)
        return pltpu.make_async_copy(src.at[rows], dst.at[rows], sem.at[p])

    for p in range(NUM_CHUNKS):
        chunk_copy(k_hbm, kbuf, kin, p).start()
        chunk_copy(v_hbm, vbuf, vin, p).start()
    for i in range(3):
        qs[i] = jnp.swapaxes(qkv_ref[i], 0, 1)

    row = lax.broadcasted_iota(jnp.int32, (16, 128), 0)
    lane = lax.broadcasted_iota(jnp.int32, (16, 128), 1)
    head_of_row = lax.rem(row, 8)
    first = row < 8
    lane8 = lax.broadcasted_iota(jnp.int32, (8, 128), 1)

    def patch(buf, b, local, new):
        start = pl.multiple_of((local // 16) * 16, 16)
        tile = buf[b, :, pl.ds(start, 16), :].astype(F32)
        slot = lax.broadcasted_iota(jnp.int32, (8, 16, 128), 1)
        buf[b, :, pl.ds(start, 16), :] = jnp.where(slot == local - start, new[:, None, :], tile).astype(BF16)

    def spread(values, j):
        return jnp.concatenate([jnp.where(head_of_row == 2 * j, values, 0.0),
                                jnp.where(head_of_row == 2 * j + 1, values, 0.0)], axis=1).astype(BF16)

    def body(p, carry):
        mm, ll = carry
        chunk_copy(k_hbm, kbuf, kin, p).wait()
        chunk_copy(v_hbm, vbuf, vin, p).wait()
        locals_ = [pos_ref[p * CHUNK + t] - base for t in range(CHUNK)]
        for t in range(CHUNK):
            b = p * CHUNK + t
            local = locals_[t]

            @pl.when((local >= 0) & (local < BLOCK_LEN))
            def _():
                patch(kbuf, b, local, qs[1, b])
                patch(vbuf, b, local, qs[2, b])

        chunk_copy(kbuf, k_out, kdone, p).start()
        chunk_copy(vbuf, v_out, vdone, p).start()

        scores = []
        for t in range(0, CHUNK, 2):
            b = p * CHUNK + t
            query = qs[0, pl.ds(b, 2)].reshape(16, 128)
            total = None
            for j in range(4):
                keys = jnp.concatenate([jnp.concatenate([kbuf[b + e, 2 * j], kbuf[b + e, 2 * j + 1]], axis=1)
                                        for e in range(2)], axis=0)
                part = lax.dot_general(spread(query, j), keys, (((1,), (1,)), ((), ())), preferred_element_type=F32)
                total = part if total is None else total + part
            scores.append(jnp.where(first, total[:, :128], total[:, 128:]))
        weights = []
        for n, t in enumerate(range(0, CHUNK, 2)):
            b = p * CHUNK + t
            valid = lane <= jnp.where(first, locals_[t], locals_[t + 1])
            masked = jnp.where(valid, scores[n], NEG)
            top = masked.max(-1, keepdims=True)
            weight = jnp.where(valid, jnp.exp(masked - top), 0.0)
            denom = weight.sum(-1, keepdims=True)
            weights.append(weight)
            for e in range(2):
                mm = jnp.where(lane8 == b + e, top[8 * e:8 * e + 8], mm)
                ll = jnp.where(lane8 == b + e, denom[8 * e:8 * e + 8], ll)
        for n, t in enumerate(range(0, CHUNK, 2)):
            b = p * CHUNK + t
            total = None
            for j in range(4):
                vals = jnp.concatenate([vbuf[b + e, 2 * j:2 * j + 2].reshape(256, 128) for e in range(2)], axis=1)
                part = jnp.dot(spread(weights[n], j), vals, preferred_element_type=F32)
                total = part if total is None else total + part
            o_ref[pl.ds(b, 2)] = jnp.where(first, total[:, :128], total[:, 128:]).reshape(2, 8, 128)
        return mm, ll

    zeros = jnp.zeros((8, 128), F32)
    mm, ll = lax.fori_loop(0, NUM_CHUNKS, body, (zeros, zeros))
    st_ref[0] = mm
    st_ref[1] = ll
    for p in range(NUM_CHUNKS):
        chunk_copy(kbuf, k_out, kdone, p).wait()
        chunk_copy(vbuf, v_out, vdone, p).wait()


def attn_call(positions, qkv, k_cache, v_cache):
    cache = jax.ShapeDtypeStruct(k_cache.shape, BF16)
    return pl.pallas_call(
        attn_kernel,
        out_shape=(cache, cache, jax.ShapeDtypeStruct((ROWS, HEADS, HEAD_DIM), F32),
                   jax.ShapeDtypeStruct((2, HEADS, 128), F32)),
        in_specs=[pl.BlockSpec(memory_space=pltpu.SMEM), vmem_spec(), any_spec(), any_spec()],
        out_specs=(any_spec(), any_spec(), vmem_spec(), vmem_spec()),
        scratch_shapes=[
            pltpu.VMEM(k_cache.shape, BF16),
            pltpu.VMEM(k_cache.shape, BF16),
            pltpu.VMEM((3, ROWS, HEADS, HEAD_DIM), F32),
            pltpu.SemaphoreType.DMA((NUM_CHUNKS,)),
            pltpu.SemaphoreType.DMA((NUM_CHUNKS,)),
            pltpu.SemaphoreType.DMA((NUM_CHUNKS,)),
            pltpu.SemaphoreType.DMA((NUM_CHUNKS,)),
        ],
        compiler_params=pltpu.CompilerParams(vmem_limit_bytes=24 * MIB),
        name='attn',
    )(positions, qkv, k_cache, v_cache)


SEND_ORDER = (3, 2, 1)


def finish_kernel(o_ref, st_ref, hid_hbm, bo_hbm, g_hbm, b_hbm, b1_hbm, b2_hbm, wo_hbm, w1_hbm, w2_hbm, out_ref,
                  hid_ref, bo_buf, g_buf, b_buf, b1_buf, b2_buf, rows_ref, small_sem,
                  wo_buf, w1_buf, w2_buf, c1_o, c1_s, cs_o, cs_s, c2_o, c2_s, a_f32, a_bf, rs_send, rs_recv,
                  m_own, m_send, m_recv, gat, y_bf, u_bf,
                  wo_sem, w1_sem, w2_sem, c_ssem, c_rsem, rs_ssem, rs_rsem, m_ssem, m_rsem, g_ssem, g_rsem):
    z = lax.axis_index('tp')
    sp = lax.axis_index('sp')
    core = lax.rem(sp, 2)
    yy = sp // 2
    partner = sp + 1 - 2 * core
    across = lax.rem(sp + 2, 4)
    across_other = lax.rem(partner + 2, 4)
    zpeer = {1: z + 1 - 2 * lax.rem(z, 2), 2: lax.rem(z + 2, 4), 3: 3 - z, 0: z}

    smalls = [pltpu.make_async_copy(src, dst, small_sem.at[n]) for n, (src, dst) in enumerate((
        (hid_hbm, hid_ref), (bo_hbm, bo_buf), (g_hbm, g_buf), (b_hbm, b_buf), (b1_hbm, b1_buf), (b2_hbm, b2_buf)))]
    for copy in smalls:
        copy.start()
    loads = []
    for j in range(4):
        loads.append(pltpu.make_async_copy(wo_hbm.at[:, dyn(yy * 2048 + j * 512, 512)], wo_buf.at[j], wo_sem.at[j]))
    for j in range(4):
        loads.append(pltpu.make_async_copy(w1_hbm.at[:, dyn(core * 2048 + j * 512, 512)], w1_buf.at[j], w1_sem.at[j]))
    for j in range(4):
        loads.append(pltpu.make_async_copy(w2_hbm.at[dyn(core * 2048, 2048), dyn(yy * 2048 + j * 512, 512)],
                                           w2_buf.at[j], w2_sem.at[j]))
    for load in loads:
        load.start()

    barrier = pltpu.get_barrier_semaphore()
    for k in (1, 2, 3):
        pl.semaphore_signal(barrier, inc=1, device_id={'tp': zpeer[k]}, device_id_type=MESH)
    for peer in (partner, across, across_other):
        pl.semaphore_signal(barrier, inc=1, device_id={'sp': peer}, device_id_type=MESH)
    pl.semaphore_wait(barrier, 6)

    def own_lanes(x):
        return jnp.where(core == 0, x, pltpu.roll(x, 112, 1))

    c1 = (remote(o_ref.at[dyn((1 - core) * HALF_ROWS, HALF_ROWS)], c1_o, c_ssem.at[0], c_rsem.at[0], {'sp': partner}),
          remote(st_ref, c1_s, c_ssem.at[1], c_rsem.at[1], {'sp': partner}))
    for copy in c1:
        copy.start()
    for copy in smalls:
        copy.wait()
    for n, buf in enumerate((bo_buf, g_buf, b_buf, b1_buf, b2_buf)):
        rows_ref[n] = as_row(buf)
    m_a, l_a = own_lanes(st_ref[0]), own_lanes(st_ref[1])
    for copy in c1:
        copy.wait_recv()
    m_b, l_b = own_lanes(c1_s[0]), own_lanes(c1_s[1])
    m_ab = jnp.maximum(m_a, m_b)
    f_a, f_b = jnp.exp(m_a - m_ab), jnp.exp(m_b - m_ab)
    l_ab = f_a * l_a + f_b * l_b
    cs_s[0] = m_ab
    cs_s[1] = l_ab
    for t in range(HALF_ROWS):
        cs_o[t] = o_ref[core * HALF_ROWS + t] * f_a[:, t:t + 1] + c1_o[t] * f_b[:, t:t + 1]

    c2 = (remote(cs_s, c2_s, c_ssem.at[2], c_rsem.at[2], {'sp': across}),
          remote(cs_o, c2_o, c_ssem.at[3], c_rsem.at[3], {'sp': across}))
    for copy in c2:
        copy.start()
    c2[0].wait_recv()
    m_c, l_c = c2_s[0], c2_s[1]
    m_all = jnp.maximum(m_ab, m_c)
    f_ab, f_c = jnp.exp(m_ab - m_all), jnp.exp(m_c - m_all)
    denom = f_ab * l_ab + f_c * l_c
    c2[1].wait_recv()
    for t in range(HALF_ROWS):
        mixed = cs_o[t] * f_ab[:, t:t + 1] + c2_o[t] * f_c[:, t:t + 1]
        a_f32[t] = mixed / denom[:, t:t + 1]
    for h in range(HEADS):
        a_bf[:, h * 128:(h + 1) * 128] = a_f32[:, h, :].astype(BF16)

    def scatter(ar, n, k):
        return remote(rs_send.at[ar, n], rs_recv.at[ar, n], rs_ssem.at[ar, n], rs_rsem.at[ar, n], {'tp': zpeer[k]})

    def gathered(ar, s, zz, n, device):
        return remote(gat.at[ar, s, zz], gat.at[ar, s, zz], g_ssem.at[ar, n], g_rsem.at[ar, s, zz], device)

    def share(ar, block):
        gat[ar, sp, z] = block
        sends = [gathered(ar, sp, z, n, {'tp': zpeer[k]}) for n, k in enumerate(SEND_ORDER)]
        for copy in sends:
            copy.start()

        def pass_on(zz, n):
            out = [gathered(ar, sp, zz, n + i, {'sp': peer}) for i, peer in enumerate((across, across_other, partner))]
            for copy in out:
                copy.start()
            return out

        sends += pass_on(z, 3)
        for i, k in enumerate((1, 2, 3)):
            gathered(ar, sp, zpeer[k], 0, {'tp': zpeer[k]}).wait_recv()
            sends += pass_on(zpeer[k], 6 + 3 * i)
        for k in (0, 1, 2, 3):
            for peer in (partner, across, across_other):
                gathered(ar, peer, zpeer[k], 0, {'sp': peer}).wait_recv()
        return sends

    row0 = core * HALF_ROWS
    col0 = yy * 2048 + z * 512
    my_rows = dyn(row0, HALF_ROWS)
    my_cols = dyn(col0, 512)

    for j in range(4):
        loads[j].wait()
    pending = []
    for n, k in enumerate(SEND_ORDER):
        rs_send[0, n] = jnp.dot(a_bf[...], wo_buf[zpeer[k]], preferred_element_type=F32)
        copy = scatter(0, n, k)
        copy.start()
        pending.append(copy)
    total = jnp.dot(a_bf[...], wo_buf[z], preferred_element_type=F32)
    for copy in pending:
        copy.wait_recv()
    total = total + rs_recv[0, 0] + rs_recv[0, 1] + rs_recv[0, 2]
    resid = (hid_ref[my_rows, my_cols].astype(F32) + total + rows_ref[0, :, my_cols]).astype(BF16).astype(F32)
    pending += share(0, resid)

    for c in range(2):
        slots = [(2 * y + c, zz) for y in range(2) for zz in range(4)]
        acc = None
        for s, zz in slots:
            acc = gat[0, s, zz] if acc is None else acc + gat[0, s, zz]
        mean = jnp.sum(acc, -1, keepdims=True) * (1.0 / DIM)
        acc = None
        for s, zz in slots:
            centered = gat[0, s, zz] - mean
            acc = centered * centered if acc is None else acc + centered * centered
        scale = lax.rsqrt(jnp.sum(acc, -1, keepdims=True) * (1.0 / DIM) + LN_EPS)
        for s, zz in slots:
            cols = pl.ds((s // 2) * 2048 + zz * 512, 512)
            y_bf[c * 16:(c + 1) * 16, cols] = ((gat[0, s, zz] - mean) * scale * rows_ref[1, :, cols]
                                               + rows_ref[2, :, cols]).astype(BF16)

    for j in range(4):
        loads[4 + j].wait()
        part = jnp.dot(y_bf[...], w1_buf[j], preferred_element_type=F32)
        part = part + rows_ref[3, :, dyn(core * 2048 + j * 512, 512)]
        u_bf[:, j * 512:(j + 1) * 512] = jnp.maximum(part, 0.0).astype(BF16)
    for j in range(4):
        loads[8 + j].wait()
    swaps = []
    scatters = []

    def merge(n):
        swaps[n].wait_recv()
        merged = m_own[n] + m_recv[n]
        if n < 3:
            rs_send[1, n] = merged
            copy = scatter(1, n, SEND_ORDER[n])
            copy.start()
            scatters.append(copy)
        return merged

    for n, k in enumerate(SEND_ORDER + (0,)):
        part = jnp.dot(u_bf[...], w2_buf[zpeer[k]], preferred_element_type=F32)
        m_send[n] = jnp.where(core == 0, part[16:], part[:16])
        m_own[n] = jnp.where(core == 0, part[:16], part[16:])
        copy = remote(m_send.at[n], m_recv.at[n], m_ssem.at[n], m_rsem.at[n], {'sp': partner})
        copy.start()
        swaps.append(copy)
        if n >= 2:
            merge(n - 2)
    merge(2)
    total = merge(3)
    for copy in scatters:
        copy.wait_recv()
    total = total + rs_recv[1, 0] + rs_recv[1, 1] + rs_recv[1, 2]
    final = (resid + total + rows_ref[4, :, my_cols]).astype(BF16).astype(F32)
    pending += share(1, final)
    for s in range(4):
        for zz in range(4):
            out_ref[(s % 2) * 16:(s % 2) * 16 + 16, (s // 2) * 2048 + zz * 512:(s // 2) * 2048 + zz * 512 + 512] = (
                gat[1, s, zz].astype(BF16))

    for copy in (*c1, *c2, *pending, *swaps, *scatters):
        copy.wait_send()


def finish_call(o_part, stats, hidden, b_out, gain, bias, b_fc1, b_fc2, w_out, w_fc1, w_fc2):
    dma = pltpu.SemaphoreType.DMA
    return pl.pallas_call(
        finish_kernel,
        out_shape=jax.ShapeDtypeStruct((ROWS, DIM), BF16),
        in_specs=[vmem_spec()] * 2 + [any_spec()] * 9,
        out_specs=vmem_spec(),
        scratch_shapes=[
            pltpu.VMEM((ROWS, DIM), BF16),
            *[pltpu.VMEM((DIM,), BF16) for _ in range(5)],
            pltpu.VMEM((5, 1, DIM), F32),
            dma((6,)),
            pltpu.VMEM((4, 1024, 512), BF16),
            pltpu.VMEM((4, DIM, 512), BF16),
            pltpu.VMEM((4, 2048, 512), BF16),
            pltpu.VMEM((16, 8, 128), F32), pltpu.VMEM((2, 8, 128), F32),
            pltpu.VMEM((16, 8, 128), F32), pltpu.VMEM((2, 8, 128), F32),
            pltpu.VMEM((16, 8, 128), F32), pltpu.VMEM((2, 8, 128), F32),
            pltpu.VMEM((16, 8, 128), F32),
            pltpu.VMEM((16, 1024), BF16),
            pltpu.VMEM((2, 3, 16, 512), F32), pltpu.VMEM((2, 3, 16, 512), F32),
            pltpu.VMEM((4, 16, 512), F32), pltpu.VMEM((4, 16, 512), F32), pltpu.VMEM((4, 16, 512), F32),
            pltpu.VMEM((2, 4, 4, 16, 512), F32),
            pltpu.VMEM((ROWS, DIM), BF16),
            pltpu.VMEM((ROWS, 2048), BF16),
            dma((4,)), dma((4,)), dma((4,)), dma((4,)), dma((4,)), dma((2, 3)), dma((2, 3)),
            dma((4,)), dma((4,)), dma((2, 15)), dma((2, 4, 4)),
        ],
        compiler_params=pltpu.CompilerParams(collective_id=1, has_side_effects=True, vmem_limit_bytes=44 * MIB),
        name='finish',
    )(o_part, stats, hidden, b_out, gain, bias, b_fc1, b_fc2, w_out, w_fc1, w_fc2)


def solution(mesh):
    cache_spec = P('dp', 'tp', 'sp', None)
    col_spec = P(None, 'tp')
    row_spec = P('tp', None)
    in_specs = (P('dp', None), P('dp'), cache_spec, cache_spec, P(), P(), col_spec, P('tp'), col_spec, P('tp'),
                col_spec, P('tp'), row_spec, P(), P(), P(), col_spec, P('tp'), row_spec, P())
    out_specs = (P('dp', None), cache_spec, cache_spec)

    def local_layer(hidden, positions, k_cache, v_cache, ln1_gain, ln1_bias, w_query, b_query, w_key, b_key, w_value, b_value, w_out, b_out, ln2_gain, ln2_bias, w_fc1, b_fc1, w_fc2, b_fc2):
        keep = lambda array: pltpu.with_memory_space_constraint(array, pltpu.HBM)
        qkv = qkv_call(*map(keep, (hidden, ln1_gain, ln1_bias, w_query, b_query, w_key, b_key, w_value, b_value)))
        k_next, v_next, o_part, stats = attn_call(positions, qkv, keep(k_cache), keep(v_cache))
        result = finish_call(o_part, stats, *map(keep, (hidden, b_out, ln2_gain, ln2_bias, b_fc1, b_fc2, w_out, w_fc1, w_fc2)))
        return result, k_next, v_next

    return jax.shard_map(local_layer, mesh=mesh, in_specs=in_specs, out_specs=out_specs, check_vma=False)
```

```python
import jax
import jax.numpy as jnp
from jax import lax
from jax.experimental import pallas as pl
from jax.experimental.pallas import tpu as pltpu
from jax.sharding import PartitionSpec as P

LN_EPS = 1e-5
NEG = -1e30
F32 = jnp.float32
BF16 = jnp.bfloat16
MESH = pl.DeviceIdType.MESH
ROWS = 32
HALF_ROWS = 16
DIM = 4096
HEADS = 8
HEAD_DIM = 128
BLOCK_LEN = 128
MIB = 1 << 20

def any_spec():
    return pl.BlockSpec(memory_space=pltpu.HBM)

def vmem_spec():
    return pl.BlockSpec(memory_space=pltpu.VMEM)

def remote(src, dst, send_sem, recv_sem, device):
    return pltpu.make_async_remote_copy(src_ref=src, dst_ref=dst, send_sem=send_sem, recv_sem=recv_sem,
                                        device_id=device, device_id_type=MESH)

def dyn(start, size):
    return pl.ds(pl.multiple_of(start, size), size)

QKV_CHUNKS = 4
QKV_ROWS = DIM // QKV_CHUNKS

def as_row(vec_ref):
    return vec_ref[...].astype(F32)[None, :]

def qkv_kernel(h_hbm, g_hbm, b_hbm, wq_ref, wk_ref, wv_ref, bq_hbm, bk_hbm, bv_hbm, k_hbm, out_ref, k_vmem,
               h_buf, g_buf, b_buf, bq_buf, bk_buf, bv_buf, bias_rows, wbuf, norm, send, recv, vsem, wsem, ksem, ssem, rsem):
    smalls = [pltpu.make_async_copy(src, dst, vsem.at[n]) for n, (src, dst) in enumerate((
        (h_hbm, h_buf), (g_hbm, g_buf), (b_hbm, b_buf), (bq_hbm, bq_buf), (bk_hbm, bk_buf), (bv_hbm, bv_buf)))]
    for copy in smalls:
        copy.start()
    sp = lax.axis_index('sp')
    core = lax.rem(sp, 2)
    partner = sp + 1 - 2 * core
    cols = dyn(core * 512, 512)
    copies = []
    for i, weight in enumerate((wq_ref, wk_ref, wv_ref)):
        for j in range(QKV_CHUNKS):
            rows = pl.ds(j * QKV_ROWS, QKV_ROWS)
            copy = pltpu.make_async_copy(weight.at[rows, cols], wbuf.at[i, rows, :], wsem.at[i, j])
            copy.start(priority=1)
            copies.append(copy)
    prefetch = []
    for j in range(4):
        rows = pl.ds(j * 8, 8)
        copy = pltpu.make_async_copy(k_hbm.at[rows], k_vmem.at[rows], ksem.at[j])
        copy.start(priority=1)
        prefetch.append(copy)
    barrier = pltpu.get_barrier_semaphore()
    pl.semaphore_signal(barrier, inc=1, device_id={'sp': partner}, device_id_type=MESH)

    for copy in smalls:
        copy.wait()

    values = h_buf[...].astype(F32)
    centered = values - jnp.mean(values, -1, keepdims=True)
    variance = jnp.mean(centered * centered, -1, keepdims=True)
    norm[...] = (centered * lax.rsqrt(variance + LN_EPS) * as_row(g_buf) + as_row(b_buf)).astype(BF16)
    for i, buf in enumerate((bq_buf, bk_buf, bv_buf)):
        bias_rows[i] = as_row(buf)

    pl.semaphore_wait(barrier, 1)

    sends = []
    for i in range(3):
        total = None
        for j in range(QKV_CHUNKS):
            copies[i * QKV_CHUNKS + j].wait()
            rows = pl.ds(j * QKV_ROWS, QKV_ROWS)
            part = jnp.dot(norm[:, rows], wbuf[i, rows, :], preferred_element_type=F32)
            total = part if total is None else total + part
        total = total + bias_rows[i, :, cols]
        if i == 0:
            total = total * HEAD_DIM ** -0.5
        total = total.astype(BF16).astype(F32)
        for h in range(4):
            send[i, h] = total[:, h * 128:(h + 1) * 128]
        copy = remote(send.at[i], recv.at[i], ssem.at[i], rsem.at[i], {'sp': partner})
        copy.start()
        sends.append(copy)
        for h in range(4):
            out_ref[i, core * 4 + h] = total[:, h * 128:(h + 1) * 128]

    for i in range(3):
        sends[i].wait_recv()
        for h in range(4):
            out_ref[i, (1 - core) * 4 + h] = recv[i, h]

    for i in range(3):
        sends[i].wait_send()
    for copy in prefetch:
        copy.wait()

def qkv_call(hidden, gain, bias, w_query, b_query, w_key, b_key, w_value, b_value, k_cache):
    return pl.pallas_call(
        qkv_kernel,
        out_shape=(jax.ShapeDtypeStruct((3, HEADS, ROWS, HEAD_DIM), F32), pltpu.VMEM(k_cache.shape, BF16)),
        in_specs=[any_spec()] * 10,
        out_specs=(vmem_spec(), vmem_spec()),
        scratch_shapes=[
            pltpu.VMEM((ROWS, DIM), BF16),
            pltpu.VMEM((DIM,), BF16), pltpu.VMEM((DIM,), BF16),
            pltpu.VMEM((1024,), BF16), pltpu.VMEM((1024,), BF16), pltpu.VMEM((1024,), BF16),
            pltpu.VMEM((3, 1, 1024), F32),
            pltpu.VMEM((3, DIM, 512), BF16),
            pltpu.VMEM((ROWS, DIM), BF16),
            pltpu.VMEM((3, 4, ROWS, 128), F32),
            pltpu.VMEM((3, 4, ROWS, 128), F32),
            pltpu.SemaphoreType.DMA((6,)),
            pltpu.SemaphoreType.DMA((3, QKV_CHUNKS)),
            pltpu.SemaphoreType.DMA((4,)),
            pltpu.SemaphoreType.DMA((3,)),
            pltpu.SemaphoreType.DMA((3,)),
        ],
        compiler_params=pltpu.CompilerParams(collective_id=0, has_side_effects=True, vmem_limit_bytes=16 * MIB),
        name='qkv',
    )(hidden, gain, bias, w_query, w_key, w_value, b_query, b_key, b_value, k_cache)

CHUNK = 4
NUM_CHUNKS = ROWS // CHUNK

def attn_kernel(pos_ref, qkv_ref, k_in, v_hbm, k_out, v_out, o_ref, st_ref, kbuf, vbuf, qs, vin, kdone, vdone):
    base = lax.axis_index('sp') * BLOCK_LEN

    def chunk_copy(src, dst, sem, p):
        rows = pl.ds(p * CHUNK, CHUNK)
        return pltpu.make_async_copy(src.at[rows], dst.at[rows], sem.at[p])

    for p in range(NUM_CHUNKS):
        chunk_copy(v_hbm, vbuf, vin, p).start()

    for i in range(3):
        qs[i] = jnp.swapaxes(qkv_ref[i], 0, 1)

    row = lax.broadcasted_iota(jnp.int32, (16, 128), 0)
    lane = lax.broadcasted_iota(jnp.int32, (16, 128), 1)
    head_of_row = lax.rem(row, 8)
    first = row < 8
    lane8 = lax.broadcasted_iota(jnp.int32, (8, 128), 1)

    def patch(buf, b, local, new):
        start = pl.multiple_of((local // 16) * 16, 16)
        tile = buf[b, :, pl.ds(start, 16), :].astype(F32)
        slot = lax.broadcasted_iota(jnp.int32, (8, 16, 128), 1)
        buf[b, :, pl.ds(start, 16), :] = jnp.where(slot == local - start, new[:, None, :], tile).astype(BF16)

    def spread(values, j):
        return jnp.concatenate([jnp.where(head_of_row == 2 * j, values, 0.0),
                                jnp.where(head_of_row == 2 * j + 1, values, 0.0)], axis=1).astype(BF16)

    def body(p, carry):
        mm, ll = carry
        chunk_copy(v_hbm, vbuf, vin, p).wait()
        locals_ = [pos_ref[p * CHUNK + t] - base for t in range(CHUNK)]
        for t in range(CHUNK):
            b = p * CHUNK + t
            local = locals_[t]

            @pl.when((local >= 0) & (local < BLOCK_LEN))
            def _():
                patch(kbuf, b, local, qs[1, b])
                patch(vbuf, b, local, qs[2, b])

        chunk_copy(kbuf, k_out, kdone, p).start()
        chunk_copy(vbuf, v_out, vdone, p).start()

        scores = []
        for t in range(0, CHUNK, 2):
            b = p * CHUNK + t
            query = qs[0, pl.ds(b, 2)].reshape(16, 128)
            total = None
            for j in range(4):
                keys = jnp.concatenate([jnp.concatenate([kbuf[b + e, 2 * j], kbuf[b + e, 2 * j + 1]], axis=1)
                                        for e in range(2)], axis=0)
                part = lax.dot_general(spread(query, j), keys, (((1,), (1,)), ((), ())), preferred_element_type=F32)
                total = part if total is None else total + part
            scores.append(jnp.where(first, total[:, :128], total[:, 128:]))
        weights = []
        for n, t in enumerate(range(0, CHUNK, 2)):
            b = p * CHUNK + t
            valid = lane <= jnp.where(first, locals_[t], locals_[t + 1])
            masked = jnp.where(valid, scores[n], NEG)
            top = masked.max(-1, keepdims=True)
            weight = jnp.where(valid, jnp.exp(masked - top), 0.0)
            denom = weight.sum(-1, keepdims=True)
            weights.append(weight)
            for e in range(2):
                mm = jnp.where(lane8 == b + e, top[8 * e:8 * e + 8], mm)
                ll = jnp.where(lane8 == b + e, denom[8 * e:8 * e + 8], ll)
        for n, t in enumerate(range(0, CHUNK, 2)):
            b = p * CHUNK + t
            total = None
            for j in range(4):
                vals = jnp.concatenate([vbuf[b + e, 2 * j:2 * j + 2].reshape(256, 128) for e in range(2)], axis=1)
                part = jnp.dot(spread(weights[n], j), vals, preferred_element_type=F32)
                total = part if total is None else total + part
            o_ref[pl.ds(b, 2)] = jnp.where(first, total[:, :128], total[:, 128:]).reshape(2, 8, 128)
        return mm, ll

    zeros = jnp.zeros((8, 128), F32)
    mm, ll = lax.fori_loop(0, NUM_CHUNKS, body, (zeros, zeros))
    st_ref[0] = mm
    st_ref[1] = ll

    for p in range(NUM_CHUNKS):
        chunk_copy(kbuf, k_out, kdone, p).wait()
        chunk_copy(vbuf, v_out, vdone, p).wait()

def attn_call(positions, qkv, k_cache, v_cache):
    cache = jax.ShapeDtypeStruct(k_cache.shape, BF16)
    return pl.pallas_call(
        attn_kernel,
        out_shape=(cache, cache, jax.ShapeDtypeStruct((ROWS, HEADS, HEAD_DIM), F32),
                   jax.ShapeDtypeStruct((2, HEADS, 128), F32), pltpu.VMEM(k_cache.shape, BF16)),
        in_specs=[pl.BlockSpec(memory_space=pltpu.SMEM), vmem_spec(), vmem_spec(), any_spec()],
        out_specs=(any_spec(), any_spec(), vmem_spec(), vmem_spec(), vmem_spec()),
        input_output_aliases={2: 4},
        scratch_shapes=[
            pltpu.VMEM(k_cache.shape, BF16),
            pltpu.VMEM((3, ROWS, HEADS, HEAD_DIM), F32),
            pltpu.SemaphoreType.DMA((NUM_CHUNKS,)),
            pltpu.SemaphoreType.DMA((NUM_CHUNKS,)),
            pltpu.SemaphoreType.DMA((NUM_CHUNKS,)),
        ],
        compiler_params=pltpu.CompilerParams(vmem_limit_bytes=16 * MIB),
        name='attn',
    )(positions, qkv, k_cache, v_cache)

SEND_ORDER = (3, 2, 1)

def finish_kernel(o_ref, st_ref, hid_hbm, bo_hbm, g_hbm, b_hbm, b1_hbm, b2_hbm, wo_hbm, w1_hbm, w2_hbm, out_ref,
                  hid_ref, bo_buf, g_buf, b_buf, b1_buf, b2_buf, rows_ref, small_sem,
                  wo_buf, w1_buf, w2_buf, c1_o, c1_s, cs_o, cs_s, c2_o, c2_s, a_f32, a_bf, rs_send, rs_recv,
                  m_own, m_send, m_recv, gat, y_bf, u_bf,
                  wo_sem, w1_sem, w2_sem, c_ssem, c_rsem, rs_ssem, rs_rsem, m_ssem, m_rsem, g_ssem, g_rsem):
    z = lax.axis_index('tp')
    sp = lax.axis_index('sp')
    core = lax.rem(sp, 2)
    yy = sp // 2
    partner = sp + 1 - 2 * core
    across = lax.rem(sp + 2, 4)
    across_other = lax.rem(partner + 2, 4)
    zpeer = {1: z + 1 - 2 * lax.rem(z, 2), 2: lax.rem(z + 2, 4), 3: 3 - z, 0: z}

    smalls = [pltpu.make_async_copy(src, dst, small_sem.at[n]) for n, (src, dst) in enumerate((
        (hid_hbm, hid_ref), (bo_hbm, bo_buf), (g_hbm, g_buf), (b_hbm, b_buf), (b1_hbm, b1_buf), (b2_hbm, b2_buf)))]
    for copy in smalls:
        copy.start()
    inner = (z == 0) | (z == 3)
    nearest = (zpeer[1], jnp.where(inner, zpeer[3], zpeer[2]), jnp.where(inner, zpeer[2], zpeer[3]))
    loads = []
    for j in range(4):
        loads.append(pltpu.make_async_copy(wo_hbm.at[:, dyn(yy * 2048 + j * 512, 512)], wo_buf.at[j], wo_sem.at[j]))
    for j in range(4):
        loads.append(pltpu.make_async_copy(w1_hbm.at[:, dyn(core * 2048 + j * 512, 512)], w1_buf.at[j], w1_sem.at[j]))
    for j in range(4):
        loads.append(pltpu.make_async_copy(w2_hbm.at[dyn(core * 2048, 2048), dyn(yy * 2048 + j * 512, 512)],
                                           w2_buf.at[j], w2_sem.at[j]))
    barrier = pltpu.get_barrier_semaphore()
    for k in (1, 2, 3):
        pl.semaphore_signal(barrier, inc=1, device_id={'tp': zpeer[k]}, device_id_type=MESH)
    for peer in (partner, across, across_other):
        pl.semaphore_signal(barrier, inc=1, device_id={'sp': peer}, device_id_type=MESH)

    pl.semaphore_wait(barrier, 6)

    def own_lanes(x):
        return jnp.where(core == 0, x, pltpu.roll(x, 112, 1))

    c1 = (remote(o_ref.at[dyn((1 - core) * HALF_ROWS, HALF_ROWS)], c1_o, c_ssem.at[0], c_rsem.at[0], {'sp': partner}),
          remote(st_ref, c1_s, c_ssem.at[1], c_rsem.at[1], {'sp': partner}))
    for copy in c1:
        copy.start()
    for load in loads[:4]:
        load.start(priority=1)
    for copy in smalls:
        copy.wait()
    for n, buf in enumerate((bo_buf, g_buf, b_buf, b1_buf, b2_buf)):
        rows_ref[n] = as_row(buf)
    m_a, l_a = own_lanes(st_ref[0]), own_lanes(st_ref[1])
    for copy in c1:
        copy.wait_recv()
    m_b, l_b = own_lanes(c1_s[0]), own_lanes(c1_s[1])
    m_ab = jnp.maximum(m_a, m_b)
    f_a, f_b = jnp.exp(m_a - m_ab), jnp.exp(m_b - m_ab)
    l_ab = f_a * l_a + f_b * l_b
    cs_s[0] = m_ab
    cs_s[1] = l_ab
    for t in range(HALF_ROWS):
        cs_o[t] = o_ref[core * HALF_ROWS + t] * f_a[:, t:t + 1] + c1_o[t] * f_b[:, t:t + 1]

    c2 = (remote(cs_s, c2_s, c_ssem.at[2], c_rsem.at[2], {'sp': across}),
          remote(cs_o, c2_o, c_ssem.at[3], c_rsem.at[3], {'sp': across}))
    for copy in c2:
        copy.start()
    for load in loads[4:6]:
        load.start(priority=1)
    c2[0].wait_recv()
    m_c, l_c = c2_s[0], c2_s[1]

    m_all = jnp.maximum(m_ab, m_c)
    f_ab, f_c = jnp.exp(m_ab - m_all), jnp.exp(m_c - m_all)
    denom = f_ab * l_ab + f_c * l_c
    c2[1].wait_recv()
    for t in range(HALF_ROWS):
        mixed = cs_o[t] * f_ab[:, t:t + 1] + c2_o[t] * f_c[:, t:t + 1]
        a_f32[t] = mixed / denom[:, t:t + 1]
    for h in range(HEADS):
        a_bf[:, h * 128:(h + 1) * 128] = a_f32[:, h, :].astype(BF16)

    def scatter(ar, n, k):
        return remote(rs_send.at[ar, n], rs_recv.at[ar, n], rs_ssem.at[ar, n], rs_rsem.at[ar, n], {'tp': zpeer[k]})

    def gathered(ar, s, zz, n, device):
        return remote(gat.at[ar, s, zz], gat.at[ar, s, zz], g_ssem.at[ar, n], g_rsem.at[ar, s, zz], device)

    def share(ar, block):
        gat[ar, sp, z] = block
        sends = [gathered(ar, sp, z, n, {'tp': zpeer[k]}) for n, k in enumerate(SEND_ORDER)]
        for copy in sends:
            copy.start()

        def pass_on(zz, n):
            out = [gathered(ar, sp, zz, n + i, {'sp': peer}) for i, peer in enumerate((across, across_other, partner))]
            for copy in out:
                copy.start()
            return out

        sends += pass_on(z, 3)
        for i, peer in enumerate(nearest):
            gathered(ar, sp, peer, 0, {'tp': peer}).wait_recv()
            sends += pass_on(peer, 6 + 3 * i)
        for k in (0, 1, 2, 3):
            for peer in (partner, across, across_other):
                gathered(ar, peer, zpeer[k], 0, {'sp': peer}).wait_recv()
        return sends

    row0 = core * HALF_ROWS
    col0 = yy * 2048 + z * 512
    my_rows = dyn(row0, HALF_ROWS)
    my_cols = dyn(col0, 512)

    for j in range(4):
        loads[j].wait()
    pending = []
    for n, k in enumerate(SEND_ORDER):
        rs_send[0, n] = jnp.dot(a_bf[...], wo_buf[zpeer[k]], preferred_element_type=F32)
        copy = scatter(0, n, k)
        copy.start()
        pending.append(copy)
    for load in loads[6:8]:
        load.start(priority=1)
    total = jnp.dot(a_bf[...], wo_buf[z], preferred_element_type=F32)

    for copy in pending:
        copy.wait_recv()
    total = total + rs_recv[0, 0] + rs_recv[0, 1] + rs_recv[0, 2]
    resid = (hid_ref[my_rows, my_cols].astype(F32) + total + rows_ref[0, :, my_cols]).astype(BF16).astype(F32)

    pending += share(0, resid)

    for load in loads[8:]:
        load.start(priority=1)
    for c in range(2):
        slots = [(2 * y + c, zz) for y in range(2) for zz in range(4)]
        acc = None
        for s, zz in slots:
            acc = gat[0, s, zz] if acc is None else acc + gat[0, s, zz]
        mean = jnp.sum(acc, -1, keepdims=True) * (1.0 / DIM)
        acc = None
        for s, zz in slots:
            centered = gat[0, s, zz] - mean
            acc = centered * centered if acc is None else acc + centered * centered
        scale = lax.rsqrt(jnp.sum(acc, -1, keepdims=True) * (1.0 / DIM) + LN_EPS)
        for s, zz in slots:
            cols = pl.ds((s // 2) * 2048 + zz * 512, 512)
            y_bf[c * 16:(c + 1) * 16, cols] = ((gat[0, s, zz] - mean) * scale * rows_ref[1, :, cols]
                                               + rows_ref[2, :, cols]).astype(BF16)

    for j in range(4):
        loads[4 + j].wait()
        part = jnp.dot(y_bf[...], w1_buf[j], preferred_element_type=F32)
        part = part + rows_ref[3, :, dyn(core * 2048 + j * 512, 512)]
        u_bf[:, j * 512:(j + 1) * 512] = jnp.maximum(part, 0.0).astype(BF16)

    for j in range(4):
        loads[8 + j].wait()
    swaps = []
    scatters = []

    def merge(n):
        swaps[n].wait_recv()
        merged = m_own[n] + m_recv[n]
        if n < 3:
            rs_send[1, n] = merged
            copy = scatter(1, n, SEND_ORDER[n])
            copy.start()
            scatters.append(copy)
        return merged

    for n, k in enumerate(SEND_ORDER + (0,)):
        part = jnp.dot(u_bf[...], w2_buf[zpeer[k]], preferred_element_type=F32)
        m_send[n] = jnp.where(core == 0, part[16:], part[:16])
        m_own[n] = jnp.where(core == 0, part[:16], part[16:])
        copy = remote(m_send.at[n], m_recv.at[n], m_ssem.at[n], m_rsem.at[n], {'sp': partner})
        copy.start()
        swaps.append(copy)
        if n >= 2:
            merge(n - 2)
    merge(2)
    total = merge(3)

    for copy in scatters:
        copy.wait_recv()
    total = total + rs_recv[1, 0] + rs_recv[1, 1] + rs_recv[1, 2]
    final = (resid + total + rows_ref[4, :, my_cols]).astype(BF16).astype(F32)

    pending += share(1, final)

    for s in range(4):
        for zz in range(4):
            out_ref[(s % 2) * 16:(s % 2) * 16 + 16, (s // 2) * 2048 + zz * 512:(s // 2) * 2048 + zz * 512 + 512] = (
                gat[1, s, zz].astype(BF16))

    for copy in (*c1, *c2, *pending, *swaps, *scatters):
        copy.wait_send()

def finish_call(o_part, stats, hidden, b_out, gain, bias, b_fc1, b_fc2, w_out, w_fc1, w_fc2):
    dma = pltpu.SemaphoreType.DMA
    return pl.pallas_call(
        finish_kernel,
        out_shape=jax.ShapeDtypeStruct((ROWS, DIM), BF16),
        in_specs=[vmem_spec()] * 2 + [any_spec()] * 9,
        out_specs=vmem_spec(),
        scratch_shapes=[
            pltpu.VMEM((ROWS, DIM), BF16),
            *[pltpu.VMEM((DIM,), BF16) for _ in range(5)],
            pltpu.VMEM((5, 1, DIM), F32),
            dma((6,)),
            pltpu.VMEM((4, 1024, 512), BF16),
            pltpu.VMEM((4, DIM, 512), BF16),
            pltpu.VMEM((4, 2048, 512), BF16),
            pltpu.VMEM((16, 8, 128), F32), pltpu.VMEM((2, 8, 128), F32),
            pltpu.VMEM((16, 8, 128), F32), pltpu.VMEM((2, 8, 128), F32),
            pltpu.VMEM((16, 8, 128), F32), pltpu.VMEM((2, 8, 128), F32),
            pltpu.VMEM((16, 8, 128), F32),
            pltpu.VMEM((16, 1024), BF16),
            pltpu.VMEM((2, 3, 16, 512), F32), pltpu.VMEM((2, 3, 16, 512), F32),
            pltpu.VMEM((4, 16, 512), F32), pltpu.VMEM((4, 16, 512), F32), pltpu.VMEM((4, 16, 512), F32),
            pltpu.VMEM((2, 4, 4, 16, 512), F32),
            pltpu.VMEM((ROWS, DIM), BF16),
            pltpu.VMEM((ROWS, 2048), BF16),
            dma((4,)), dma((4,)), dma((4,)), dma((4,)), dma((4,)), dma((2, 3)), dma((2, 3)),
            dma((4,)), dma((4,)), dma((2, 15)), dma((2, 4, 4)),
        ],
        compiler_params=pltpu.CompilerParams(collective_id=1, has_side_effects=True, vmem_limit_bytes=44 * MIB),
        name='finish',
    )(o_part, stats, hidden, b_out, gain, bias, b_fc1, b_fc2, w_out, w_fc1, w_fc2)

def solution(mesh):
    cache_spec = P('dp', 'tp', 'sp', None)
    col_spec = P(None, 'tp')
    row_spec = P('tp', None)
    in_specs = (P('dp', None), P('dp'), cache_spec, cache_spec, P(), P(), col_spec, P('tp'), col_spec, P('tp'),
                col_spec, P('tp'), row_spec, P(), P(), P(), col_spec, P('tp'), row_spec, P())
    out_specs = (P('dp', None), cache_spec, cache_spec)

    def local_layer(hidden, positions, k_cache, v_cache, ln1_gain, ln1_bias, w_query, b_query, w_key, b_key, w_value, b_value, w_out, b_out, ln2_gain, ln2_bias, w_fc1, b_fc1, w_fc2, b_fc2):
        keep = lambda array: pltpu.with_memory_space_constraint(array, pltpu.HBM)
        qkv, k_vmem = qkv_call(*map(keep, (hidden, ln1_gain, ln1_bias, w_query, b_query, w_key, b_key, w_value, b_value, k_cache)))
        k_next, v_next, o_part, stats, _ = attn_call(positions, qkv, k_vmem, keep(v_cache))
        result = finish_call(o_part, stats, *map(keep, (hidden, b_out, ln2_gain, ln2_bias, b_fc1, b_fc2, w_out, w_fc1, w_fc2)))
        return result, k_next, v_next

    return jax.shard_map(local_layer, mesh=mesh, in_specs=in_specs, out_specs=out_specs, check_vma=False)
```

```python
import jax
import jax.numpy as jnp
from jax import lax
from jax.experimental import pallas as pl
from jax.experimental.pallas import tpu as pltpu
from jax.sharding import PartitionSpec as P

LN_EPS = 1e-5
NEG = -1e30
F32 = jnp.float32
BF16 = jnp.bfloat16
MESH = pl.DeviceIdType.MESH
ROWS = 32
HALF_ROWS = 16
DIM = 4096
HEADS = 8
HEAD_DIM = 128
BLOCK_LEN = 128
MIB = 1 << 20

def any_spec():
    return pl.BlockSpec(memory_space=pltpu.HBM)

def vmem_spec():
    return pl.BlockSpec(memory_space=pltpu.VMEM)

def remote(src, dst, send_sem, recv_sem, device):
    return pltpu.make_async_remote_copy(src_ref=src, dst_ref=dst, send_sem=send_sem, recv_sem=recv_sem,
                                        device_id=device, device_id_type=MESH)

def dyn(start, size):
    return pl.ds(pl.multiple_of(start, size), size)

QKV_CHUNKS = 4
QKV_ROWS = DIM // QKV_CHUNKS
PREFETCH_AT = (1, 3)

def as_row(vec_ref):
    return vec_ref[...].astype(F32)[None, :]

def qkv_kernel(h_hbm, g_hbm, b_hbm, wq_ref, wk_ref, wv_ref, bq_hbm, bk_hbm, bv_hbm, k_hbm, out_ref, k_vmem,
               h_buf, g_buf, b_buf, bq_buf, bk_buf, bv_buf, bias_rows, wbuf, norm, send, recv, vsem, wsem, ksem, ssem, rsem):
    smalls = [pltpu.make_async_copy(src, dst, vsem.at[n]) for n, (src, dst) in enumerate((
        (h_hbm, h_buf), (g_hbm, g_buf), (b_hbm, b_buf), (bq_hbm, bq_buf), (bk_hbm, bk_buf), (bv_hbm, bv_buf)))]
    for copy in smalls:
        copy.start()
    sp = lax.axis_index('sp')
    core = lax.rem(sp, 2)
    partner = sp + 1 - 2 * core
    cols = dyn(core * 512, 512)
    copies = []
    for i, weight in enumerate((wq_ref, wk_ref, wv_ref)):
        for j in range(QKV_CHUNKS):
            rows = pl.ds(j * QKV_ROWS, QKV_ROWS)
            copy = pltpu.make_async_copy(weight.at[rows, cols], wbuf.at[i, rows, :], wsem.at[i, j])
            copy.start(priority=1)
            copies.append(copy)
    prefetch = []
    for j in range(4):
        rows = pl.ds(j * 8, 8)
        copy = pltpu.make_async_copy(k_hbm.at[rows], k_vmem.at[rows], ksem.at[j])
        prefetch.append(copy)
    barrier = pltpu.get_barrier_semaphore()
    pl.semaphore_signal(barrier, inc=1, device_id={'sp': partner}, device_id_type=MESH)

    for copy in smalls:
        copy.wait()

    values = h_buf[...].astype(F32)
    centered = values - jnp.mean(values, -1, keepdims=True)
    variance = jnp.mean(centered * centered, -1, keepdims=True)
    norm[...] = (centered * lax.rsqrt(variance + LN_EPS) * as_row(g_buf) + as_row(b_buf)).astype(BF16)
    for i, buf in enumerate((bq_buf, bk_buf, bv_buf)):
        bias_rows[i] = as_row(buf)

    pl.semaphore_wait(barrier, 1)

    sends = []
    for i in range(3):
        total = None
        for j in range(QKV_CHUNKS):
            copies[i * QKV_CHUNKS + j].wait()
            if (i, j) == PREFETCH_AT:
                for copy in prefetch:
                    copy.start(priority=1)
            rows = pl.ds(j * QKV_ROWS, QKV_ROWS)
            part = jnp.dot(norm[:, rows], wbuf[i, rows, :], preferred_element_type=F32)
            total = part if total is None else total + part
        total = total + bias_rows[i, :, cols]
        if i == 0:
            total = total * HEAD_DIM ** -0.5
        total = total.astype(BF16).astype(F32)
        for h in range(4):
            send[i, h] = total[:, h * 128:(h + 1) * 128]
        copy = remote(send.at[i], recv.at[i], ssem.at[i], rsem.at[i], {'sp': partner})
        copy.start()
        sends.append(copy)
        for h in range(4):
            out_ref[i, core * 4 + h] = total[:, h * 128:(h + 1) * 128]

    for i in range(3):
        sends[i].wait_recv()
        for h in range(4):
            out_ref[i, (1 - core) * 4 + h] = recv[i, h]

    for i in range(3):
        sends[i].wait_send()
    for copy in prefetch:
        copy.wait()

def qkv_call(hidden, gain, bias, w_query, b_query, w_key, b_key, w_value, b_value, k_cache):
    return pl.pallas_call(
        qkv_kernel,
        out_shape=(jax.ShapeDtypeStruct((3, HEADS, ROWS, HEAD_DIM), F32), pltpu.VMEM(k_cache.shape, BF16)),
        in_specs=[any_spec()] * 10,
        out_specs=(vmem_spec(), vmem_spec()),
        scratch_shapes=[
            pltpu.VMEM((ROWS, DIM), BF16),
            pltpu.VMEM((DIM,), BF16), pltpu.VMEM((DIM,), BF16),
            pltpu.VMEM((1024,), BF16), pltpu.VMEM((1024,), BF16), pltpu.VMEM((1024,), BF16),
            pltpu.VMEM((3, 1, 1024), F32),
            pltpu.VMEM((3, DIM, 512), BF16),
            pltpu.VMEM((ROWS, DIM), BF16),
            pltpu.VMEM((3, 4, ROWS, 128), F32),
            pltpu.VMEM((3, 4, ROWS, 128), F32),
            pltpu.SemaphoreType.DMA((6,)),
            pltpu.SemaphoreType.DMA((3, QKV_CHUNKS)),
            pltpu.SemaphoreType.DMA((4,)),
            pltpu.SemaphoreType.DMA((3,)),
            pltpu.SemaphoreType.DMA((3,)),
        ],
        compiler_params=pltpu.CompilerParams(collective_id=0, has_side_effects=True, vmem_limit_bytes=16 * MIB),
        name='qkv',
    )(hidden, gain, bias, w_query, w_key, w_value, b_query, b_key, b_value, k_cache)

CHUNK = 4
NUM_CHUNKS = ROWS // CHUNK

def attn_kernel(pos_ref, qkv_ref, k_in, v_hbm, k_out, v_out, o_ref, st_ref, kbuf, vbuf, qs, vin, kdone, vdone):
    base = lax.axis_index('sp') * BLOCK_LEN

    def chunk_copy(src, dst, sem, p):
        rows = pl.ds(p * CHUNK, CHUNK)
        return pltpu.make_async_copy(src.at[rows], dst.at[rows], sem.at[p])

    for p in range(NUM_CHUNKS):
        chunk_copy(v_hbm, vbuf, vin, p).start()

    for i in range(3):
        qs[i] = jnp.swapaxes(qkv_ref[i], 0, 1)

    row = lax.broadcasted_iota(jnp.int32, (16, 128), 0)
    lane = lax.broadcasted_iota(jnp.int32, (16, 128), 1)
    head_of_row = lax.rem(row, 8)
    first = row < 8
    lane8 = lax.broadcasted_iota(jnp.int32, (8, 128), 1)

    def patch(buf, b, local, new):
        start = pl.multiple_of((local // 16) * 16, 16)
        tile = buf[b, :, pl.ds(start, 16), :].astype(F32)
        slot = lax.broadcasted_iota(jnp.int32, (8, 16, 128), 1)
        buf[b, :, pl.ds(start, 16), :] = jnp.where(slot == local - start, new[:, None, :], tile).astype(BF16)

    def spread(values, j):
        return jnp.concatenate([jnp.where(head_of_row == 2 * j, values, 0.0),
                                jnp.where(head_of_row == 2 * j + 1, values, 0.0)], axis=1).astype(BF16)

    def body(p, carry):
        mm, ll = carry
        chunk_copy(v_hbm, vbuf, vin, p).wait()
        locals_ = [pos_ref[p * CHUNK + t] - base for t in range(CHUNK)]
        for t in range(CHUNK):
            b = p * CHUNK + t
            local = locals_[t]

            @pl.when((local >= 0) & (local < BLOCK_LEN))
            def _():
                patch(kbuf, b, local, qs[1, b])
                patch(vbuf, b, local, qs[2, b])

        chunk_copy(kbuf, k_out, kdone, p).start()
        chunk_copy(vbuf, v_out, vdone, p).start()

        scores = []
        for t in range(0, CHUNK, 2):
            b = p * CHUNK + t
            query = qs[0, pl.ds(b, 2)].reshape(16, 128)
            total = None
            for j in range(4):
                keys = jnp.concatenate([jnp.concatenate([kbuf[b + e, 2 * j], kbuf[b + e, 2 * j + 1]], axis=1)
                                        for e in range(2)], axis=0)
                part = lax.dot_general(spread(query, j), keys, (((1,), (1,)), ((), ())), preferred_element_type=F32)
                total = part if total is None else total + part
            scores.append(jnp.where(first, total[:, :128], total[:, 128:]))
        weights = []
        for n, t in enumerate(range(0, CHUNK, 2)):
            b = p * CHUNK + t
            valid = lane <= jnp.where(first, locals_[t], locals_[t + 1])
            masked = jnp.where(valid, scores[n], NEG)
            top = masked.max(-1, keepdims=True)
            weight = jnp.where(valid, jnp.exp(masked - top), 0.0)
            denom = weight.sum(-1, keepdims=True)
            weights.append(weight)
            for e in range(2):
                mm = jnp.where(lane8 == b + e, top[8 * e:8 * e + 8], mm)
                ll = jnp.where(lane8 == b + e, denom[8 * e:8 * e + 8], ll)
        for n, t in enumerate(range(0, CHUNK, 2)):
            b = p * CHUNK + t
            total = None
            for j in range(4):
                vals = jnp.concatenate([vbuf[b + e, 2 * j:2 * j + 2].reshape(256, 128) for e in range(2)], axis=1)
                part = jnp.dot(spread(weights[n], j), vals, preferred_element_type=F32)
                total = part if total is None else total + part
            o_ref[pl.ds(b, 2)] = jnp.where(first, total[:, :128], total[:, 128:]).reshape(2, 8, 128)
        return mm, ll

    zeros = jnp.zeros((8, 128), F32)
    mm, ll = lax.fori_loop(0, NUM_CHUNKS, body, (zeros, zeros))
    st_ref[0] = mm
    st_ref[1] = ll

    for p in range(NUM_CHUNKS):
        chunk_copy(kbuf, k_out, kdone, p).wait()
        chunk_copy(vbuf, v_out, vdone, p).wait()

def attn_call(positions, qkv, k_cache, v_cache):
    cache = jax.ShapeDtypeStruct(k_cache.shape, BF16)
    return pl.pallas_call(
        attn_kernel,
        out_shape=(cache, cache, jax.ShapeDtypeStruct((ROWS, HEADS, HEAD_DIM), F32),
                   jax.ShapeDtypeStruct((2, HEADS, 128), F32), pltpu.VMEM(k_cache.shape, BF16)),
        in_specs=[pl.BlockSpec(memory_space=pltpu.SMEM), vmem_spec(), vmem_spec(), any_spec()],
        out_specs=(any_spec(), any_spec(), vmem_spec(), vmem_spec(), vmem_spec()),
        input_output_aliases={2: 4},
        scratch_shapes=[
            pltpu.VMEM(k_cache.shape, BF16),
            pltpu.VMEM((3, ROWS, HEADS, HEAD_DIM), F32),
            pltpu.SemaphoreType.DMA((NUM_CHUNKS,)),
            pltpu.SemaphoreType.DMA((NUM_CHUNKS,)),
            pltpu.SemaphoreType.DMA((NUM_CHUNKS,)),
        ],
        compiler_params=pltpu.CompilerParams(vmem_limit_bytes=16 * MIB),
        name='attn',
    )(positions, qkv, k_cache, v_cache)

SEND_INNER = (2, 3, 1)
SEND_OUTER = (1, 2, 3)

def finish_kernel(o_ref, st_ref, hid_hbm, bo_hbm, g_hbm, b_hbm, b1_hbm, b2_hbm, wo_hbm, w1_hbm, w2_hbm, out_ref,
                  hid_ref, bo_buf, g_buf, b_buf, b1_buf, b2_buf, rows_ref, small_sem,
                  wo_buf, w1_buf, w2_buf, c1_o, c1_s, cs_o, cs_s, c2_o, c2_s, a_f32, a_bf, rs_send, rs_recv,
                  u_send, u_recv, gat, gat2, y_bf, u_bf, x_bf,
                  wo_sem, w1_sem, w2_sem, c_ssem, c_rsem, rs_ssem, rs_rsem, m_ssem, m_rsem,
                  g_ssem, g_rsem, g2_ssem, g2_rsem):
    z = lax.axis_index('tp')
    sp = lax.axis_index('sp')
    core = lax.rem(sp, 2)
    yy = sp // 2
    partner = sp + 1 - 2 * core
    across = lax.rem(sp + 2, 4)
    across_other = lax.rem(partner + 2, 4)
    zpeer = {1: z + 1 - 2 * lax.rem(z, 2), 2: lax.rem(z + 2, 4), 3: 3 - z}
    inner = (z == 0) | (z == 3)
    step = [jnp.where(inner, a, b) for a, b in zip(SEND_INNER, SEND_OUTER)]
    target = [jnp.where(inner, zpeer[a], zpeer[b]) for a, b in zip(SEND_INNER, SEND_OUTER)]
    nearest = (zpeer[1], jnp.where(inner, zpeer[3], zpeer[2]), jnp.where(inner, zpeer[2], zpeer[3]))

    smalls = [pltpu.make_async_copy(src, dst, small_sem.at[n]) for n, (src, dst) in enumerate((
        (hid_hbm, hid_ref), (bo_hbm, bo_buf), (g_hbm, g_buf), (b_hbm, b_buf), (b1_hbm, b1_buf), (b2_hbm, b2_buf)))]
    for copy in smalls:
        copy.start()
    wo_loads, w1_loads, w2_loads = [], [], []
    for j in range(4):
        cols = dyn(core * 2048 + j * 512, 512)
        wo_loads.append(pltpu.make_async_copy(wo_hbm.at[:, cols], wo_buf.at[j], wo_sem.at[j]))
        w1_loads.append(pltpu.make_async_copy(w1_hbm.at[:, cols], w1_buf.at[j], w1_sem.at[j]))
    for half, rows in enumerate((core, 1 - core)):
        for n, dest in enumerate((*target, z)):
            w2_loads.append(pltpu.make_async_copy(
                w2_hbm.at[dyn(rows * 2048, 2048), dyn(core * 2048 + dest * 512, 512)],
                w2_buf.at[half, n], w2_sem.at[half, n]))

    def begin(loads):
        for load in loads:
            load.start(priority=1)

    barrier = pltpu.get_barrier_semaphore()
    for k in (1, 2, 3):
        pl.semaphore_signal(barrier, inc=1, device_id={'tp': zpeer[k]}, device_id_type=MESH)
    for peer in (partner, across, across_other):
        pl.semaphore_signal(barrier, inc=1, device_id={'sp': peer}, device_id_type=MESH)

    pl.semaphore_wait(barrier, 6)

    def own_lanes(x):
        return jnp.where(yy == 0, x, pltpu.roll(x, 112, 1))

    c1 = (remote(st_ref, c1_s, c_ssem.at[0], c_rsem.at[0], {'sp': across}),
          remote(o_ref.at[dyn((1 - yy) * HALF_ROWS, HALF_ROWS)], c1_o, c_ssem.at[1], c_rsem.at[1], {'sp': across}))
    for copy in c1:
        copy.start()
    begin(wo_loads)
    begin(w1_loads[:1])
    for copy in smalls:
        copy.wait()
    for n, buf in enumerate((bo_buf, g_buf, b_buf, b1_buf, b2_buf)):
        rows_ref[n] = as_row(buf)
    m_a, l_a = own_lanes(st_ref[0]), own_lanes(st_ref[1])
    c1[0].wait_recv()
    m_b, l_b = own_lanes(c1_s[0]), own_lanes(c1_s[1])
    m_ab = jnp.maximum(m_a, m_b)
    f_a, f_b = jnp.exp(m_a - m_ab), jnp.exp(m_b - m_ab)
    l_ab = f_a * l_a + f_b * l_b
    cs_s[0] = m_ab
    cs_s[1] = l_ab
    c1[1].wait_recv()
    for t in range(HALF_ROWS):
        cs_o[t] = o_ref[yy * HALF_ROWS + t] * f_a[:, t:t + 1] + c1_o[t] * f_b[:, t:t + 1]

    c2 = (remote(cs_s, c2_s, c_ssem.at[2], c_rsem.at[2], {'sp': partner}),
          remote(cs_o, c2_o, c_ssem.at[3], c_rsem.at[3], {'sp': partner}))
    for copy in c2:
        copy.start()
    begin(w1_loads[1:2])
    c2[0].wait_recv()
    m_c, l_c = c2_s[0], c2_s[1]
    m_all = jnp.maximum(m_ab, m_c)
    f_ab, f_c = jnp.exp(m_ab - m_all), jnp.exp(m_c - m_all)
    inv = 1.0 / (f_ab * l_ab + f_c * l_c)
    f_ab, f_c = f_ab * inv, f_c * inv
    c2[1].wait_recv()
    for t in range(HALF_ROWS):
        a_f32[t] = cs_o[t] * f_ab[:, t:t + 1] + c2_o[t] * f_c[:, t:t + 1]
    for h in range(HEADS):
        a_bf[:, h * 128:(h + 1) * 128] = a_f32[:, h, :].astype(BF16)

    def scatter(ar, n):
        return remote(rs_send.at[ar, n], rs_recv.at[ar, step[n] - 1], rs_ssem.at[ar, n],
                      rs_rsem.at[ar, step[n] - 1], {'tp': target[n]})

    def in_plane(c, zz, n, device):
        return remote(gat.at[c, zz], gat.at[c, zz], g_ssem.at[n], g_rsem.at[c, zz], device)

    def in_group(s, zz, n, device):
        return remote(gat2.at[s, zz], gat2.at[s, zz], g2_ssem.at[n], g2_rsem.at[s, zz], device)

    my_rows = dyn(yy * HALF_ROWS, HALF_ROWS)
    my_cols = dyn(core * 2048 + z * 512, 512)

    for load in wo_loads:
        load.wait()
    pending = []
    for n in range(3):
        rs_send[0, n] = jnp.dot(a_bf[...], wo_buf[target[n]], preferred_element_type=F32)
        copy = scatter(0, n)
        copy.start()
        pending.append(copy)
    begin(w1_loads[2:])
    total = jnp.dot(a_bf[...], wo_buf[z], preferred_element_type=F32)
    resid = hid_ref[my_rows, my_cols].astype(F32) + rows_ref[0, :, my_cols] + total

    for copy in pending[:3]:
        copy.wait_recv()
    resid = (resid + (rs_recv[0, 0] + rs_recv[0, 1] + rs_recv[0, 2])).astype(BF16).astype(F32)

    gat[core, z] = resid
    sends = [in_plane(core, z, n, {'tp': target[n]}) for n in range(3)] + [in_plane(core, z, 3, {'sp': partner})]
    for copy in sends:
        copy.start()
    begin(w2_loads[:2])
    for i, peer in enumerate(nearest):
        in_plane(core, peer, 0, {'tp': peer}).wait_recv()
        copy = in_plane(core, peer, 4 + i, {'sp': partner})
        copy.start()
        sends.append(copy)
    for zz in (z, *nearest):
        in_plane(1 - core, zz, 0, {'sp': partner}).wait_recv()
    pending += sends

    begin(w2_loads[2:])
    slots = [(c, zz) for c in range(2) for zz in range(4)]
    acc = None
    for c, zz in slots:
        acc = gat[c, zz] if acc is None else acc + gat[c, zz]
    mean = jnp.sum(acc, -1, keepdims=True) * (1.0 / DIM)
    acc = None
    for c, zz in slots:
        centered = gat[c, zz] - mean
        acc = centered * centered if acc is None else acc + centered * centered
    scale = lax.rsqrt(jnp.sum(acc, -1, keepdims=True) * (1.0 / DIM) + LN_EPS)
    for c, zz in slots:
        cols = pl.ds(c * 2048 + zz * 512, 512)
        y_bf[:, cols] = ((gat[c, zz] - mean) * scale * rows_ref[1, :, cols] + rows_ref[2, :, cols]).astype(BF16)

    swaps = []
    for j in range(4):
        w1_loads[j].wait()
        part = jnp.dot(y_bf[...], w1_buf[j], preferred_element_type=F32)
        part = part + rows_ref[3, :, dyn(core * 2048 + j * 512, 512)]
        act = jnp.maximum(part, 0.0).astype(BF16)
        u_bf[:, j * 512:(j + 1) * 512] = act
        u_send[j] = act.astype(F32)
        copy = remote(u_send.at[j], u_recv.at[j], m_ssem.at[j], m_rsem.at[j], {'sp': partner})
        copy.start()
        swaps.append(copy)

    own = []
    for n in range(4):
        w2_loads[n].wait()
        own.append(jnp.dot(u_bf[...], w2_buf[0, n], preferred_element_type=F32))
    for j in range(4):
        swaps[j].wait_recv()
        x_bf[:, j * 512:(j + 1) * 512] = u_recv[j].astype(BF16)
    scatters = []
    for n in range(4):
        w2_loads[4 + n].wait()
        total = own[n] + jnp.dot(x_bf[...], w2_buf[1, n], preferred_element_type=F32)
        if n < 3:
            rs_send[1, n] = total
            copy = scatter(1, n)
            copy.start()
            scatters.append(copy)
    final = resid + rows_ref[4, :, my_cols] + total

    for copy in scatters:
        copy.wait_recv()
    final = (final + (rs_recv[1, 0] + rs_recv[1, 1] + rs_recv[1, 2])).astype(BF16).astype(F32)

    gat2[sp, z] = final
    sends = [in_group(sp, z, n, {'tp': target[n]}) for n in range(3)]
    for copy in sends:
        copy.start()

    def pass_on(zz, n):
        out = [in_group(sp, zz, n + i, {'sp': peer}) for i, peer in enumerate((across, across_other, partner))]
        for copy in out:
            copy.start()
        return out

    sends += pass_on(z, 3)
    for i, peer in enumerate(nearest):
        in_group(sp, peer, 0, {'tp': peer}).wait_recv()
        sends += pass_on(peer, 6 + 3 * i)
    for zz in (z, *nearest):
        for peer in (partner, across, across_other):
            in_group(peer, zz, 0, {'sp': peer}).wait_recv()
    pending += sends

    for s in range(4):
        for zz in range(4):
            start = (s % 2) * 2048 + zz * 512
            out_ref[(s // 2) * 16:(s // 2) * 16 + 16, start:start + 512] = gat2[s, zz].astype(BF16)

    for copy in (*c1, *c2, *pending, *swaps, *scatters):
        copy.wait_send()

def finish_call(o_part, stats, hidden, b_out, gain, bias, b_fc1, b_fc2, w_out, w_fc1, w_fc2):
    dma = pltpu.SemaphoreType.DMA
    return pl.pallas_call(
        finish_kernel,
        out_shape=jax.ShapeDtypeStruct((ROWS, DIM), BF16),
        in_specs=[vmem_spec()] * 2 + [any_spec()] * 9,
        out_specs=vmem_spec(),
        scratch_shapes=[
            pltpu.VMEM((ROWS, DIM), BF16),
            *[pltpu.VMEM((DIM,), BF16) for _ in range(5)],
            pltpu.VMEM((5, 1, DIM), F32),
            dma((6,)),
            pltpu.VMEM((4, 1024, 512), BF16),
            pltpu.VMEM((4, DIM, 512), BF16),
            pltpu.VMEM((2, 4, 2048, 512), BF16),
            pltpu.VMEM((16, 8, 128), F32), pltpu.VMEM((2, 8, 128), F32),
            pltpu.VMEM((16, 8, 128), F32), pltpu.VMEM((2, 8, 128), F32),
            pltpu.VMEM((16, 8, 128), F32), pltpu.VMEM((2, 8, 128), F32),
            pltpu.VMEM((16, 8, 128), F32),
            pltpu.VMEM((16, 1024), BF16),
            pltpu.VMEM((2, 3, 16, 512), F32), pltpu.VMEM((2, 3, 16, 512), F32),
            pltpu.VMEM((4, 16, 512), F32), pltpu.VMEM((4, 16, 512), F32),
            pltpu.VMEM((2, 4, 16, 512), F32), pltpu.VMEM((4, 4, 16, 512), F32),
            pltpu.VMEM((16, DIM), BF16),
            pltpu.VMEM((16, 2048), BF16), pltpu.VMEM((16, 2048), BF16),
            dma((4,)), dma((4,)), dma((2, 4)), dma((4,)), dma((4,)), dma((2, 3)), dma((2, 3)),
            dma((4,)), dma((4,)), dma((7,)), dma((2, 4)), dma((15,)), dma((4, 4)),
        ],
        compiler_params=pltpu.CompilerParams(collective_id=1, has_side_effects=True, vmem_limit_bytes=48 * MIB),
        name='finish',
    )(o_part, stats, hidden, b_out, gain, bias, b_fc1, b_fc2, w_out, w_fc1, w_fc2)

def solution(mesh):
    cache_spec = P('dp', 'tp', 'sp', None)
    col_spec = P(None, 'tp')
    row_spec = P('tp', None)
    in_specs = (P('dp', None), P('dp'), cache_spec, cache_spec, P(), P(), col_spec, P('tp'), col_spec, P('tp'),
                col_spec, P('tp'), row_spec, P(), P(), P(), col_spec, P('tp'), row_spec, P())
    out_specs = (P('dp', None), cache_spec, cache_spec)

    def local_layer(hidden, positions, k_cache, v_cache, ln1_gain, ln1_bias, w_query, b_query, w_key, b_key, w_value, b_value, w_out, b_out, ln2_gain, ln2_bias, w_fc1, b_fc1, w_fc2, b_fc2):
        keep = lambda array: pltpu.with_memory_space_constraint(array, pltpu.HBM)
        qkv, k_vmem = qkv_call(*map(keep, (hidden, ln1_gain, ln1_bias, w_query, b_query, w_key, b_key, w_value, b_value, k_cache)))
        k_next, v_next, o_part, stats, _ = attn_call(positions, qkv, k_vmem, keep(v_cache))
        result = finish_call(o_part, stats, *map(keep, (hidden, b_out, ln2_gain, ln2_bias, b_fc1, b_fc2, w_out, w_fc1, w_fc2)))
        return result, k_next, v_next

    return jax.shard_map(local_layer, mesh=mesh, in_specs=in_specs, out_specs=out_specs, check_vma=False)
```

```python
import jax
import jax.numpy as jnp
from jax import lax
from jax.experimental import pallas as pl
from jax.experimental.pallas import tpu as pltpu
from jax.sharding import PartitionSpec as P

LN_EPS = 1e-5
NEG = -1e30
F32 = jnp.float32
BF16 = jnp.bfloat16
MESH = pl.DeviceIdType.MESH
ROWS = 32
HALF_ROWS = 16
DIM = 4096
HEADS = 8
HEAD_DIM = 128
BLOCK_LEN = 128
MIB = 1 << 20

def any_spec():
    return pl.BlockSpec(memory_space=pltpu.HBM)

def vmem_spec():
    return pl.BlockSpec(memory_space=pltpu.VMEM)

def remote(src, dst, send_sem, recv_sem, device):
    return pltpu.make_async_remote_copy(src_ref=src, dst_ref=dst, send_sem=send_sem, recv_sem=recv_sem,
                                        device_id=device, device_id_type=MESH)

def dyn(start, size):
    return pl.ds(pl.multiple_of(start, size), size)

QKV_CHUNKS = 4
QKV_ROWS = DIM // QKV_CHUNKS
PREFETCH_AT = (1, 3)

def as_row(vec_ref):
    return vec_ref[...].astype(F32)[None, :]

def qkv_kernel(h_hbm, g_hbm, b_hbm, wq_ref, wk_ref, wv_ref, bq_hbm, bk_hbm, bv_hbm, k_hbm, out_ref, k_vmem,
               h_buf, g_buf, b_buf, bq_buf, bk_buf, bv_buf, bias_rows, wbuf, norm, send, recv, vsem, wsem, ksem, ssem, rsem):
    smalls = [pltpu.make_async_copy(src, dst, vsem.at[n]) for n, (src, dst) in enumerate((
        (h_hbm, h_buf), (g_hbm, g_buf), (b_hbm, b_buf), (bq_hbm, bq_buf), (bk_hbm, bk_buf), (bv_hbm, bv_buf)))]
    for copy in smalls:
        copy.start()
    sp = lax.axis_index('sp')
    core = lax.rem(sp, 2)
    partner = sp + 1 - 2 * core
    cols = dyn(core * 512, 512)
    copies = []
    for i, weight in enumerate((wq_ref, wk_ref, wv_ref)):
        for j in range(QKV_CHUNKS):
            rows = pl.ds(j * QKV_ROWS, QKV_ROWS)
            copy = pltpu.make_async_copy(weight.at[rows, cols], wbuf.at[i, rows, :], wsem.at[i, j])
            copy.start(priority=1)
            copies.append(copy)
    prefetch = []
    for j in range(4):
        rows = pl.ds(j * 8, 8)
        copy = pltpu.make_async_copy(k_hbm.at[rows], k_vmem.at[rows], ksem.at[j])
        prefetch.append(copy)
    barrier = pltpu.get_barrier_semaphore()
    pl.semaphore_signal(barrier, inc=1, device_id={'sp': partner}, device_id_type=MESH)

    for copy in smalls:
        copy.wait()

    values = h_buf[...].astype(F32)
    centered = values - jnp.mean(values, -1, keepdims=True)
    variance = jnp.mean(centered * centered, -1, keepdims=True)
    norm[...] = (centered * lax.rsqrt(variance + LN_EPS) * as_row(g_buf) + as_row(b_buf)).astype(BF16)
    for i, buf in enumerate((bq_buf, bk_buf, bv_buf)):
        bias_rows[i] = as_row(buf)

    pl.semaphore_wait(barrier, 1)

    sends = []
    for i in range(3):
        total = None
        for j in range(QKV_CHUNKS):
            copies[i * QKV_CHUNKS + j].wait()
            if (i, j) == PREFETCH_AT:
                for copy in prefetch:
                    copy.start(priority=1)
            rows = pl.ds(j * QKV_ROWS, QKV_ROWS)
            part = jnp.dot(norm[:, rows], wbuf[i, rows, :], preferred_element_type=F32)
            total = part if total is None else total + part
        total = total + bias_rows[i, :, cols]
        if i == 0:
            total = total * HEAD_DIM ** -0.5
        total = total.astype(BF16).astype(F32)
        for h in range(4):
            send[i, h] = total[:, h * 128:(h + 1) * 128]
        copy = remote(send.at[i], recv.at[i], ssem.at[i], rsem.at[i], {'sp': partner})
        copy.start()
        sends.append(copy)
        for h in range(4):
            out_ref[i, core * 4 + h] = total[:, h * 128:(h + 1) * 128]

    for i in range(3):
        sends[i].wait_recv()
        for h in range(4):
            out_ref[i, (1 - core) * 4 + h] = recv[i, h]

    for i in range(3):
        sends[i].wait_send()
    for copy in prefetch:
        copy.wait()

def qkv_call(hidden, gain, bias, w_query, b_query, w_key, b_key, w_value, b_value, k_cache):
    return pl.pallas_call(
        qkv_kernel,
        out_shape=(jax.ShapeDtypeStruct((3, HEADS, ROWS, HEAD_DIM), F32), pltpu.VMEM(k_cache.shape, BF16)),
        in_specs=[any_spec()] * 10,
        out_specs=(vmem_spec(), vmem_spec()),
        scratch_shapes=[
            pltpu.VMEM((ROWS, DIM), BF16),
            pltpu.VMEM((DIM,), BF16), pltpu.VMEM((DIM,), BF16),
            pltpu.VMEM((1024,), BF16), pltpu.VMEM((1024,), BF16), pltpu.VMEM((1024,), BF16),
            pltpu.VMEM((3, 1, 1024), F32),
            pltpu.VMEM((3, DIM, 512), BF16),
            pltpu.VMEM((ROWS, DIM), BF16),
            pltpu.VMEM((3, 4, ROWS, 128), F32),
            pltpu.VMEM((3, 4, ROWS, 128), F32),
            pltpu.SemaphoreType.DMA((6,)),
            pltpu.SemaphoreType.DMA((3, QKV_CHUNKS)),
            pltpu.SemaphoreType.DMA((4,)),
            pltpu.SemaphoreType.DMA((3,)),
            pltpu.SemaphoreType.DMA((3,)),
        ],
        compiler_params=pltpu.CompilerParams(collective_id=0, has_side_effects=True, vmem_limit_bytes=16 * MIB),
        name='qkv',
    )(hidden, gain, bias, w_query, w_key, w_value, b_query, b_key, b_value, k_cache)

CHUNK = 4
NUM_CHUNKS = ROWS // CHUNK

def attn_kernel(pos_hbm, qkv_ref, k_in, v_hbm, k_out, v_out, o_ref, st_ref, kbuf, vbuf, qs, pos_ref, pos_sem, vin, kdone, vdone):
    base = lax.axis_index('sp') * BLOCK_LEN
    pos_copy = pltpu.make_async_copy(pos_hbm, pos_ref, pos_sem)
    pos_copy.start()

    def chunk_copy(src, dst, sem, p):
        rows = pl.ds(p * CHUNK, CHUNK)
        return pltpu.make_async_copy(src.at[rows], dst.at[rows], sem.at[p])

    for p in range(NUM_CHUNKS):
        chunk_copy(v_hbm, vbuf, vin, p).start()

    for i in range(3):
        qs[i] = jnp.swapaxes(qkv_ref[i], 0, 1)
    pos_copy.wait()

    row = lax.broadcasted_iota(jnp.int32, (16, 128), 0)
    lane = lax.broadcasted_iota(jnp.int32, (16, 128), 1)
    head_of_row = lax.rem(row, 8)
    first = row < 8
    lane8 = lax.broadcasted_iota(jnp.int32, (8, 128), 1)

    def patch(buf, b, local, new):
        start = pl.multiple_of((local // 16) * 16, 16)
        tile = buf[b, :, pl.ds(start, 16), :].astype(F32)
        slot = lax.broadcasted_iota(jnp.int32, (8, 16, 128), 1)
        buf[b, :, pl.ds(start, 16), :] = jnp.where(slot == local - start, new[:, None, :], tile).astype(BF16)

    def spread(values, j):
        return jnp.concatenate([jnp.where(head_of_row == 2 * j, values, 0.0),
                                jnp.where(head_of_row == 2 * j + 1, values, 0.0)], axis=1).astype(BF16)

    def body(p, carry):
        mm, ll = carry
        chunk_copy(v_hbm, vbuf, vin, p).wait()
        locals_ = [pos_ref[p * CHUNK + t] - base for t in range(CHUNK)]
        for t in range(CHUNK):
            b = p * CHUNK + t
            local = locals_[t]

            @pl.when((local >= 0) & (local < BLOCK_LEN))
            def _():
                patch(kbuf, b, local, qs[1, b])
                patch(vbuf, b, local, qs[2, b])

        chunk_copy(kbuf, k_out, kdone, p).start()
        chunk_copy(vbuf, v_out, vdone, p).start()

        scores = []
        for t in range(0, CHUNK, 2):
            b = p * CHUNK + t
            query = qs[0, pl.ds(b, 2)].reshape(16, 128)
            total = None
            for j in range(4):
                keys = jnp.concatenate([jnp.concatenate([kbuf[b + e, 2 * j], kbuf[b + e, 2 * j + 1]], axis=1)
                                        for e in range(2)], axis=0)
                part = lax.dot_general(spread(query, j), keys, (((1,), (1,)), ((), ())), preferred_element_type=F32)
                total = part if total is None else total + part
            scores.append(jnp.where(first, total[:, :128], total[:, 128:]))
        weights = []
        for n, t in enumerate(range(0, CHUNK, 2)):
            b = p * CHUNK + t
            valid = lane <= jnp.where(first, locals_[t], locals_[t + 1])
            masked = jnp.where(valid, scores[n], NEG)
            top = masked.max(-1, keepdims=True)
            weight = jnp.where(valid, jnp.exp(masked - top), 0.0)
            denom = weight.sum(-1, keepdims=True)
            weights.append(weight)
            for e in range(2):
                mm = jnp.where(lane8 == b + e, top[8 * e:8 * e + 8], mm)
                ll = jnp.where(lane8 == b + e, denom[8 * e:8 * e + 8], ll)
        for n, t in enumerate(range(0, CHUNK, 2)):
            b = p * CHUNK + t
            total = None
            for j in range(4):
                vals = jnp.concatenate([vbuf[b + e, 2 * j:2 * j + 2].reshape(256, 128) for e in range(2)], axis=1)
                part = jnp.dot(spread(weights[n], j), vals, preferred_element_type=F32)
                total = part if total is None else total + part
            o_ref[pl.ds(b, 2)] = jnp.where(first, total[:, :128], total[:, 128:]).reshape(2, 8, 128)
        return mm, ll

    zeros = jnp.zeros((8, 128), F32)
    mm, ll = lax.fori_loop(0, NUM_CHUNKS, body, (zeros, zeros))
    st_ref[0] = mm
    st_ref[1] = ll

    for p in range(NUM_CHUNKS):
        chunk_copy(kbuf, k_out, kdone, p).wait()
        chunk_copy(vbuf, v_out, vdone, p).wait()

def attn_call(positions, qkv, k_cache, v_cache):
    cache = jax.ShapeDtypeStruct(k_cache.shape, BF16)
    return pl.pallas_call(
        attn_kernel,
        out_shape=(cache, cache, jax.ShapeDtypeStruct((ROWS, HEADS, HEAD_DIM), F32),
                   jax.ShapeDtypeStruct((2, HEADS, 128), F32), pltpu.VMEM(k_cache.shape, BF16)),
        in_specs=[any_spec(), vmem_spec(), vmem_spec(), any_spec()],
        out_specs=(any_spec(), any_spec(), vmem_spec(), vmem_spec(), vmem_spec()),
        input_output_aliases={2: 4},
        scratch_shapes=[
            pltpu.VMEM(k_cache.shape, BF16),
            pltpu.VMEM((3, ROWS, HEADS, HEAD_DIM), F32),
            pltpu.SMEM((ROWS,), jnp.int32),
            pltpu.SemaphoreType.DMA,
            pltpu.SemaphoreType.DMA((NUM_CHUNKS,)),
            pltpu.SemaphoreType.DMA((NUM_CHUNKS,)),
            pltpu.SemaphoreType.DMA((NUM_CHUNKS,)),
        ],
        compiler_params=pltpu.CompilerParams(vmem_limit_bytes=16 * MIB),
        name='attn',
    )(positions, qkv, k_cache, v_cache)

SEND_INNER = (2, 3, 1)
SEND_OUTER = (1, 2, 3)

def finish_kernel(o_ref, st_ref, hid_hbm, bo_hbm, g_hbm, b_hbm, b1_hbm, b2_hbm, wo_hbm, w1_hbm, w2_hbm, out_ref,
                  hid_ref, bo_buf, g_buf, b_buf, b1_buf, b2_buf, rows_ref, small_sem,
                  wo_buf, w1_buf, w2_buf, c1_o, c1_s, cs_o, cs_s, c2_o, c2_s, a_f32, a_bf, rs_send, rs_recv,
                  u_send, u_recv, gat, gat2, y_bf, u_bf, x_bf,
                  wo_sem, w1_sem, w2_sem, c_ssem, c_rsem, rs_ssem, rs_rsem, m_ssem, m_rsem,
                  g_ssem, g_rsem, g2_ssem, g2_rsem):
    z = lax.axis_index('tp')
    sp = lax.axis_index('sp')
    core = lax.rem(sp, 2)
    yy = sp // 2
    partner = sp + 1 - 2 * core
    across = lax.rem(sp + 2, 4)
    across_other = lax.rem(partner + 2, 4)
    zpeer = {1: z + 1 - 2 * lax.rem(z, 2), 2: lax.rem(z + 2, 4), 3: 3 - z}
    inner = (z == 0) | (z == 3)
    step = [jnp.where(inner, a, b) for a, b in zip(SEND_INNER, SEND_OUTER)]
    target = [jnp.where(inner, zpeer[a], zpeer[b]) for a, b in zip(SEND_INNER, SEND_OUTER)]
    nearest = (zpeer[1], jnp.where(inner, zpeer[3], zpeer[2]), jnp.where(inner, zpeer[2], zpeer[3]))

    smalls = [pltpu.make_async_copy(src, dst, small_sem.at[n]) for n, (src, dst) in enumerate((
        (hid_hbm, hid_ref), (bo_hbm, bo_buf), (g_hbm, g_buf), (b_hbm, b_buf), (b1_hbm, b1_buf), (b2_hbm, b2_buf)))]
    for copy in smalls:
        copy.start()
    wo_loads, w1_loads, w2_loads = [], [], []
    for j in range(4):
        cols = dyn(core * 2048 + j * 512, 512)
        wo_loads.append(pltpu.make_async_copy(wo_hbm.at[:, cols], wo_buf.at[j], wo_sem.at[j]))
        w1_loads.append(pltpu.make_async_copy(w1_hbm.at[:, cols], w1_buf.at[j], w1_sem.at[j]))
    for half, rows in enumerate((core, 1 - core)):
        for n, dest in enumerate((*target, z)):
            w2_loads.append(pltpu.make_async_copy(
                w2_hbm.at[dyn(rows * 2048, 2048), dyn(core * 2048 + dest * 512, 512)],
                w2_buf.at[half, n], w2_sem.at[half, n]))

    def begin(loads):
        for load in loads:
            load.start(priority=1)

    barrier = pltpu.get_barrier_semaphore()
    for k in (1, 2, 3):
        pl.semaphore_signal(barrier, inc=1, device_id={'tp': zpeer[k]}, device_id_type=MESH)
    for peer in (partner, across, across_other):
        pl.semaphore_signal(barrier, inc=1, device_id={'sp': peer}, device_id_type=MESH)

    pl.semaphore_wait(barrier, 6)

    def own_lanes(x):
        return jnp.where(yy == 0, x, pltpu.roll(x, 112, 1))

    c1 = (remote(st_ref, c1_s, c_ssem.at[0], c_rsem.at[0], {'sp': across}),
          remote(o_ref.at[dyn((1 - yy) * HALF_ROWS, HALF_ROWS)], c1_o, c_ssem.at[1], c_rsem.at[1], {'sp': across}))
    for copy in c1:
        copy.start()
    begin(wo_loads)
    begin(w1_loads[:1])
    for copy in smalls:
        copy.wait()
    for n, buf in enumerate((bo_buf, g_buf, b_buf, b1_buf, b2_buf)):
        rows_ref[n] = as_row(buf)
    m_a, l_a = own_lanes(st_ref[0]), own_lanes(st_ref[1])
    c1[0].wait_recv()
    m_b, l_b = own_lanes(c1_s[0]), own_lanes(c1_s[1])
    m_ab = jnp.maximum(m_a, m_b)
    f_a, f_b = jnp.exp(m_a - m_ab), jnp.exp(m_b - m_ab)
    l_ab = f_a * l_a + f_b * l_b
    cs_s[0] = m_ab
    cs_s[1] = l_ab
    c1[1].wait_recv()
    for t in range(HALF_ROWS):
        cs_o[t] = o_ref[yy * HALF_ROWS + t] * f_a[:, t:t + 1] + c1_o[t] * f_b[:, t:t + 1]

    c2 = (remote(cs_s, c2_s, c_ssem.at[2], c_rsem.at[2], {'sp': partner}),
          remote(cs_o, c2_o, c_ssem.at[3], c_rsem.at[3], {'sp': partner}))
    for copy in c2:
        copy.start()
    begin(w1_loads[1:2])
    c2[0].wait_recv()
    m_c, l_c = c2_s[0], c2_s[1]
    m_all = jnp.maximum(m_ab, m_c)
    f_ab, f_c = jnp.exp(m_ab - m_all), jnp.exp(m_c - m_all)
    inv = 1.0 / (f_ab * l_ab + f_c * l_c)
    f_ab, f_c = f_ab * inv, f_c * inv
    c2[1].wait_recv()
    for t in range(HALF_ROWS):
        a_f32[t] = cs_o[t] * f_ab[:, t:t + 1] + c2_o[t] * f_c[:, t:t + 1]
    for h in range(HEADS):
        a_bf[:, h * 128:(h + 1) * 128] = a_f32[:, h, :].astype(BF16)

    def scatter(ar, n):
        return remote(rs_send.at[ar, n], rs_recv.at[ar, step[n] - 1], rs_ssem.at[ar, n],
                      rs_rsem.at[ar, step[n] - 1], {'tp': target[n]})

    def in_plane(c, zz, n, device):
        return remote(gat.at[c, zz], gat.at[c, zz], g_ssem.at[n], g_rsem.at[c, zz], device)

    def in_group(s, zz, n, device):
        return remote(gat2.at[s, zz], gat2.at[s, zz], g2_ssem.at[n], g2_rsem.at[s, zz], device)

    my_rows = dyn(yy * HALF_ROWS, HALF_ROWS)
    my_cols = dyn(core * 2048 + z * 512, 512)

    for load in wo_loads:
        load.wait()
    pending = []
    for n in range(3):
        rs_send[0, n] = jnp.dot(a_bf[...], wo_buf[target[n]], preferred_element_type=F32)
        copy = scatter(0, n)
        copy.start()
        pending.append(copy)
    begin(w1_loads[2:])
    total = jnp.dot(a_bf[...], wo_buf[z], preferred_element_type=F32)
    resid = hid_ref[my_rows, my_cols].astype(F32) + rows_ref[0, :, my_cols] + total

    for copy in pending[:3]:
        copy.wait_recv()
    resid = (resid + (rs_recv[0, 0] + rs_recv[0, 1] + rs_recv[0, 2])).astype(BF16).astype(F32)

    gat[core, z] = resid
    sends = [in_plane(core, z, n, {'tp': target[n]}) for n in range(3)] + [in_plane(core, z, 3, {'sp': partner})]
    for copy in sends:
        copy.start()
    begin(w2_loads[:2])
    for i, peer in enumerate(nearest):
        in_plane(core, peer, 0, {'tp': peer}).wait_recv()
        copy = in_plane(core, peer, 4 + i, {'sp': partner})
        copy.start()
        sends.append(copy)
    for zz in (z, *nearest):
        in_plane(1 - core, zz, 0, {'sp': partner}).wait_recv()
    pending += sends

    begin(w2_loads[2:])
    slots = [(c, zz) for c in range(2) for zz in range(4)]
    acc = None
    for c, zz in slots:
        acc = gat[c, zz] if acc is None else acc + gat[c, zz]
    mean = jnp.sum(acc, -1, keepdims=True) * (1.0 / DIM)
    acc = None
    for c, zz in slots:
        centered = gat[c, zz] - mean
        acc = centered * centered if acc is None else acc + centered * centered
    scale = lax.rsqrt(jnp.sum(acc, -1, keepdims=True) * (1.0 / DIM) + LN_EPS)
    for c, zz in slots:
        cols = pl.ds(c * 2048 + zz * 512, 512)
        y_bf[:, cols] = ((gat[c, zz] - mean) * scale * rows_ref[1, :, cols] + rows_ref[2, :, cols]).astype(BF16)

    swaps = []
    for j in range(4):
        w1_loads[j].wait()
        part = jnp.dot(y_bf[...], w1_buf[j], preferred_element_type=F32)
        part = part + rows_ref[3, :, dyn(core * 2048 + j * 512, 512)]
        act = jnp.maximum(part, 0.0).astype(BF16)
        u_bf[:, j * 512:(j + 1) * 512] = act
        u_send[j] = act.astype(F32)
        copy = remote(u_send.at[j], u_recv.at[j], m_ssem.at[j], m_rsem.at[j], {'sp': partner})
        copy.start()
        swaps.append(copy)

    own = []
    for n in range(4):
        w2_loads[n].wait()
        own.append(jnp.dot(u_bf[...], w2_buf[0, n], preferred_element_type=F32))
    for j in range(4):
        swaps[j].wait_recv()
        x_bf[:, j * 512:(j + 1) * 512] = u_recv[j].astype(BF16)
    scatters = []
    for n in range(4):
        w2_loads[4 + n].wait()
        total = own[n] + jnp.dot(x_bf[...], w2_buf[1, n], preferred_element_type=F32)
        if n < 3:
            rs_send[1, n] = total
            copy = scatter(1, n)
            copy.start()
            scatters.append(copy)
    final = resid + rows_ref[4, :, my_cols] + total

    for copy in scatters:
        copy.wait_recv()
    final = (final + (rs_recv[1, 0] + rs_recv[1, 1] + rs_recv[1, 2])).astype(BF16).astype(F32)

    gat2[sp, z] = final
    sends = [in_group(sp, z, n, {'tp': target[n]}) for n in range(3)]
    for copy in sends:
        copy.start()

    def pass_on(slot, zz, n, peers):
        out = [in_group(slot, zz, n + i, {'sp': peer}) for i, peer in enumerate(peers)]
        for copy in out:
            copy.start()
        return out

    def hand_on(zz, n):
        in_group(across, zz, 0, {'sp': across}).wait_recv()
        return pass_on(across, zz, n, (partner,))

    sends += pass_on(sp, z, 3, (across, partner))
    for i, peer in enumerate(nearest):
        in_group(sp, peer, 0, {'tp': peer}).wait_recv()
        if i < 2:
            sends += pass_on(sp, peer, 5 + 2 * i, (across, partner))
        else:
            sends += pass_on(sp, peer, 9, (across, across_other, partner))
        if i == 1:
            sends += hand_on(z, 12)
    for i in range(2):
        sends += hand_on(nearest[i], 13 + i)
    for zz in (z, *nearest):
        in_group(partner, zz, 0, {'sp': partner}).wait_recv()
        in_group(across_other, zz, 0, {'sp': across_other}).wait_recv()
    in_group(across, nearest[2], 0, {'sp': across}).wait_recv()
    pending += sends

    for s in range(4):
        for zz in range(4):
            start = (s % 2) * 2048 + zz * 512
            out_ref[(s // 2) * 16:(s // 2) * 16 + 16, start:start + 512] = gat2[s, zz].astype(BF16)

    for copy in (*c1, *c2, *pending, *swaps, *scatters):
        copy.wait_send()

def finish_call(o_part, stats, hidden, b_out, gain, bias, b_fc1, b_fc2, w_out, w_fc1, w_fc2):
    dma = pltpu.SemaphoreType.DMA
    return pl.pallas_call(
        finish_kernel,
        out_shape=jax.ShapeDtypeStruct((ROWS, DIM), BF16),
        in_specs=[vmem_spec()] * 2 + [any_spec()] * 9,
        out_specs=vmem_spec(),
        scratch_shapes=[
            pltpu.VMEM((ROWS, DIM), BF16),
            *[pltpu.VMEM((DIM,), BF16) for _ in range(5)],
            pltpu.VMEM((5, 1, DIM), F32),
            dma((6,)),
            pltpu.VMEM((4, 1024, 512), BF16),
            pltpu.VMEM((4, DIM, 512), BF16),
            pltpu.VMEM((2, 4, 2048, 512), BF16),
            pltpu.VMEM((16, 8, 128), F32), pltpu.VMEM((2, 8, 128), F32),
            pltpu.VMEM((16, 8, 128), F32), pltpu.VMEM((2, 8, 128), F32),
            pltpu.VMEM((16, 8, 128), F32), pltpu.VMEM((2, 8, 128), F32),
            pltpu.VMEM((16, 8, 128), F32),
            pltpu.VMEM((16, 1024), BF16),
            pltpu.VMEM((2, 3, 16, 512), F32), pltpu.VMEM((2, 3, 16, 512), F32),
            pltpu.VMEM((4, 16, 512), F32), pltpu.VMEM((4, 16, 512), F32),
            pltpu.VMEM((2, 4, 16, 512), F32), pltpu.VMEM((4, 4, 16, 512), F32),
            pltpu.VMEM((16, DIM), BF16),
            pltpu.VMEM((16, 2048), BF16), pltpu.VMEM((16, 2048), BF16),
            dma((4,)), dma((4,)), dma((2, 4)), dma((4,)), dma((4,)), dma((2, 3)), dma((2, 3)),
            dma((4,)), dma((4,)), dma((7,)), dma((2, 4)), dma((15,)), dma((4, 4)),
        ],
        compiler_params=pltpu.CompilerParams(collective_id=1, has_side_effects=True, vmem_limit_bytes=48 * MIB),
        name='finish',
    )(o_part, stats, hidden, b_out, gain, bias, b_fc1, b_fc2, w_out, w_fc1, w_fc2)

def solution(mesh):
    cache_spec = P('dp', 'tp', 'sp', None)
    col_spec = P(None, 'tp')
    row_spec = P('tp', None)
    in_specs = (P('dp', None), P('dp'), cache_spec, cache_spec, P(), P(), col_spec, P('tp'), col_spec, P('tp'),
                col_spec, P('tp'), row_spec, P(), P(), P(), col_spec, P('tp'), row_spec, P())
    out_specs = (P('dp', None), cache_spec, cache_spec)

    def local_layer(hidden, positions, k_cache, v_cache, ln1_gain, ln1_bias, w_query, b_query, w_key, b_key, w_value, b_value, w_out, b_out, ln2_gain, ln2_bias, w_fc1, b_fc1, w_fc2, b_fc2):
        keep = lambda array: pltpu.with_memory_space_constraint(array, pltpu.HBM)
        qkv, k_vmem = qkv_call(*map(keep, (hidden, ln1_gain, ln1_bias, w_query, b_query, w_key, b_key, w_value, b_value, k_cache)))
        k_next, v_next, o_part, stats, _ = attn_call(keep(positions), qkv, k_vmem, keep(v_cache))
        result = finish_call(o_part, stats, *map(keep, (hidden, b_out, ln2_gain, ln2_bias, b_fc1, b_fc2, w_out, w_fc1, w_fc2)))
        return result, k_next, v_next

    return jax.shard_map(local_layer, mesh=mesh, in_specs=in_specs, out_specs=out_specs, check_vma=False)
```

```python
import jax
import jax.numpy as jnp
from jax import lax
from jax.experimental import pallas as pl
from jax.experimental.pallas import tpu as pltpu
from jax.sharding import PartitionSpec as P

LN_EPS = 1e-5
NEG = -1e30
F32 = jnp.float32
BF16 = jnp.bfloat16
MESH = pl.DeviceIdType.MESH
ROWS = 32
HALF_ROWS = 16
DIM = 4096
HEADS = 8
HEAD_DIM = 128
BLOCK_LEN = 128
MIB = 1 << 20

def any_spec():
    return pl.BlockSpec(memory_space=pltpu.HBM)

def vmem_spec():
    return pl.BlockSpec(memory_space=pltpu.VMEM)

def remote(src, dst, send_sem, recv_sem, device):
    return pltpu.make_async_remote_copy(src_ref=src, dst_ref=dst, send_sem=send_sem, recv_sem=recv_sem,
                                        device_id=device, device_id_type=MESH)

def dyn(start, size):
    return pl.ds(pl.multiple_of(start, size), size)

QKV_CHUNKS = 4
QKV_ROWS = DIM // QKV_CHUNKS
PREFETCH_AT = (1, 3)

def as_row(vec_ref):
    return vec_ref[...].astype(F32)[None, :]

def qkv_kernel(h_hbm, g_hbm, b_hbm, wq_ref, wk_ref, wv_ref, bq_hbm, bk_hbm, bv_hbm, k_hbm, out_ref, k_vmem,
               h_buf, g_buf, b_buf, bq_buf, bk_buf, bv_buf, bias_rows, wbuf, norm, send, recv, vsem, wsem, ksem, ssem, rsem):
    smalls = [pltpu.make_async_copy(src, dst, vsem.at[n]) for n, (src, dst) in enumerate((
        (h_hbm, h_buf), (g_hbm, g_buf), (b_hbm, b_buf), (bq_hbm, bq_buf), (bk_hbm, bk_buf), (bv_hbm, bv_buf)))]
    for copy in smalls:
        copy.start()
    sp = lax.axis_index('sp')
    core = lax.rem(sp, 2)
    partner = sp + 1 - 2 * core
    cols = dyn(core * 512, 512)
    copies = []
    for i, weight in enumerate((wq_ref, wk_ref, wv_ref)):
        for j in range(QKV_CHUNKS):
            rows = pl.ds(j * QKV_ROWS, QKV_ROWS)
            copy = pltpu.make_async_copy(weight.at[rows, cols], wbuf.at[i, rows, :], wsem.at[i, j])
            copy.start(priority=1)
            copies.append(copy)
    prefetch = []
    for j in range(4):
        rows = pl.ds(j * 8, 8)
        copy = pltpu.make_async_copy(k_hbm.at[rows], k_vmem.at[rows], ksem.at[j])
        prefetch.append(copy)
    barrier = pltpu.get_barrier_semaphore()
    pl.semaphore_signal(barrier, inc=1, device_id={'sp': partner}, device_id_type=MESH)

    for copy in smalls:
        copy.wait()

    values = h_buf[...].astype(F32)
    centered = values - jnp.mean(values, -1, keepdims=True)
    variance = jnp.mean(centered * centered, -1, keepdims=True)
    norm[...] = (centered * lax.rsqrt(variance + LN_EPS) * as_row(g_buf) + as_row(b_buf)).astype(BF16)
    for i, buf in enumerate((bq_buf, bk_buf, bv_buf)):
        bias_rows[i] = as_row(buf)

    pl.semaphore_wait(barrier, 1)

    sends = []
    for i in range(3):
        total = None
        for j in range(QKV_CHUNKS):
            copies[i * QKV_CHUNKS + j].wait()
            if (i, j) == PREFETCH_AT:
                for copy in prefetch:
                    copy.start(priority=1)
            rows = pl.ds(j * QKV_ROWS, QKV_ROWS)
            part = jnp.dot(norm[:, rows], wbuf[i, rows, :], preferred_element_type=F32)
            total = part if total is None else total + part
        total = total + bias_rows[i, :, cols]
        if i == 0:
            total = total * HEAD_DIM ** -0.5
        total = total.astype(BF16).astype(F32)
        for h in range(4):
            send[i, h] = total[:, h * 128:(h + 1) * 128]
        copy = remote(send.at[i], recv.at[i], ssem.at[i], rsem.at[i], {'sp': partner})
        copy.start()
        sends.append(copy)
        for h in range(4):
            out_ref[i, core * 4 + h] = total[:, h * 128:(h + 1) * 128]

    for i in range(3):
        sends[i].wait_recv()
        for h in range(4):
            out_ref[i, (1 - core) * 4 + h] = recv[i, h]

    for i in range(3):
        sends[i].wait_send()
    for copy in prefetch:
        copy.wait()

def qkv_call(hidden, gain, bias, w_query, b_query, w_key, b_key, w_value, b_value, k_cache):
    return pl.pallas_call(
        qkv_kernel,
        out_shape=(jax.ShapeDtypeStruct((3, HEADS, ROWS, HEAD_DIM), F32), pltpu.VMEM(k_cache.shape, BF16)),
        in_specs=[any_spec()] * 10,
        out_specs=(vmem_spec(), vmem_spec()),
        scratch_shapes=[
            pltpu.VMEM((ROWS, DIM), BF16),
            pltpu.VMEM((DIM,), BF16), pltpu.VMEM((DIM,), BF16),
            pltpu.VMEM((1024,), BF16), pltpu.VMEM((1024,), BF16), pltpu.VMEM((1024,), BF16),
            pltpu.VMEM((3, 1, 1024), F32),
            pltpu.VMEM((3, DIM, 512), BF16),
            pltpu.VMEM((ROWS, DIM), BF16),
            pltpu.VMEM((3, 4, ROWS, 128), F32),
            pltpu.VMEM((3, 4, ROWS, 128), F32),
            pltpu.SemaphoreType.DMA((6,)),
            pltpu.SemaphoreType.DMA((3, QKV_CHUNKS)),
            pltpu.SemaphoreType.DMA((4,)),
            pltpu.SemaphoreType.DMA((3,)),
            pltpu.SemaphoreType.DMA((3,)),
        ],
        compiler_params=pltpu.CompilerParams(collective_id=0, has_side_effects=True, vmem_limit_bytes=16 * MIB),
        name='qkv',
    )(hidden, gain, bias, w_query, w_key, w_value, b_query, b_key, b_value, k_cache)

CHUNK = 4
NUM_CHUNKS = ROWS // CHUNK

def attn_kernel(pos_hbm, qkv_ref, k_in, v_hbm, k_out, v_out, o_ref, st_ref, kbuf, vbuf, qs, pos_ref, pos_sem, vin, kdone, vdone):
    base = lax.axis_index('sp') * BLOCK_LEN
    pos_copy = pltpu.make_async_copy(pos_hbm, pos_ref, pos_sem)
    pos_copy.start()

    def chunk_copy(src, dst, sem, p):
        rows = pl.ds(p * CHUNK, CHUNK)
        return pltpu.make_async_copy(src.at[rows], dst.at[rows], sem.at[p])

    for p in range(NUM_CHUNKS):
        chunk_copy(v_hbm, vbuf, vin, p).start()

    for i in range(3):
        qs[i] = jnp.swapaxes(qkv_ref[i], 0, 1)
    pos_copy.wait()

    row = lax.broadcasted_iota(jnp.int32, (16, 128), 0)
    lane = lax.broadcasted_iota(jnp.int32, (16, 128), 1)
    head_of_row = lax.rem(row, 8)
    first = row < 8
    lane8 = lax.broadcasted_iota(jnp.int32, (8, 128), 1)

    def patch(buf, b, local, new):
        start = pl.multiple_of((local // 16) * 16, 16)
        tile = buf[b, :, pl.ds(start, 16), :].astype(F32)
        slot = lax.broadcasted_iota(jnp.int32, (8, 16, 128), 1)
        buf[b, :, pl.ds(start, 16), :] = jnp.where(slot == local - start, new[:, None, :], tile).astype(BF16)

    def spread(values, j):
        return jnp.concatenate([jnp.where(head_of_row == 2 * j, values, 0.0),
                                jnp.where(head_of_row == 2 * j + 1, values, 0.0)], axis=1).astype(BF16)

    def body(p, carry):
        mm, ll = carry
        chunk_copy(v_hbm, vbuf, vin, p).wait()
        locals_ = [pos_ref[p * CHUNK + t] - base for t in range(CHUNK)]
        for t in range(CHUNK):
            b = p * CHUNK + t
            local = locals_[t]

            @pl.when((local >= 0) & (local < BLOCK_LEN))
            def _():
                patch(kbuf, b, local, qs[1, b])
                patch(vbuf, b, local, qs[2, b])

        chunk_copy(kbuf, k_out, kdone, p).start()
        chunk_copy(vbuf, v_out, vdone, p).start()

        scores = []
        for t in range(0, CHUNK, 2):
            b = p * CHUNK + t
            query = qs[0, pl.ds(b, 2)].reshape(16, 128)
            total = None
            for j in range(4):
                keys = jnp.concatenate([jnp.concatenate([kbuf[b + e, 2 * j], kbuf[b + e, 2 * j + 1]], axis=1)
                                        for e in range(2)], axis=0)
                part = lax.dot_general(spread(query, j), keys, (((1,), (1,)), ((), ())), preferred_element_type=F32)
                total = part if total is None else total + part
            scores.append(jnp.where(first, total[:, :128], total[:, 128:]))
        weights = []
        for n, t in enumerate(range(0, CHUNK, 2)):
            b = p * CHUNK + t
            valid = lane <= jnp.where(first, locals_[t], locals_[t + 1])
            masked = jnp.where(valid, scores[n], NEG)
            top = masked.max(-1, keepdims=True)
            weight = jnp.where(valid, jnp.exp(masked - top), 0.0)
            denom = weight.sum(-1, keepdims=True)
            weights.append(weight)
            for e in range(2):
                mm = jnp.where(lane8 == b + e, top[8 * e:8 * e + 8], mm)
                ll = jnp.where(lane8 == b + e, denom[8 * e:8 * e + 8], ll)
        for n, t in enumerate(range(0, CHUNK, 2)):
            b = p * CHUNK + t
            total = None
            for j in range(4):
                vals = jnp.concatenate([vbuf[b + e, 2 * j:2 * j + 2].reshape(256, 128) for e in range(2)], axis=1)
                part = jnp.dot(spread(weights[n], j), vals, preferred_element_type=F32)
                total = part if total is None else total + part
            o_ref[pl.ds(b, 2)] = jnp.where(first, total[:, :128], total[:, 128:]).reshape(2, 8, 128)
        return mm, ll

    zeros = jnp.zeros((8, 128), F32)
    mm, ll = lax.fori_loop(0, NUM_CHUNKS, body, (zeros, zeros))
    st_ref[0] = mm
    st_ref[1] = ll

    for p in range(NUM_CHUNKS):
        chunk_copy(kbuf, k_out, kdone, p).wait()
        chunk_copy(vbuf, v_out, vdone, p).wait()

def attn_call(positions, qkv, k_cache, v_cache):
    cache = jax.ShapeDtypeStruct(k_cache.shape, BF16)
    return pl.pallas_call(
        attn_kernel,
        out_shape=(cache, cache, jax.ShapeDtypeStruct((ROWS, HEADS, HEAD_DIM), F32),
                   jax.ShapeDtypeStruct((2, HEADS, 128), F32), pltpu.VMEM(k_cache.shape, BF16)),
        in_specs=[any_spec(), vmem_spec(), vmem_spec(), any_spec()],
        out_specs=(any_spec(), any_spec(), vmem_spec(), vmem_spec(), vmem_spec()),
        input_output_aliases={2: 4},
        scratch_shapes=[
            pltpu.VMEM(k_cache.shape, BF16),
            pltpu.VMEM((3, ROWS, HEADS, HEAD_DIM), F32),
            pltpu.SMEM((ROWS,), jnp.int32),
            pltpu.SemaphoreType.DMA,
            pltpu.SemaphoreType.DMA((NUM_CHUNKS,)),
            pltpu.SemaphoreType.DMA((NUM_CHUNKS,)),
            pltpu.SemaphoreType.DMA((NUM_CHUNKS,)),
        ],
        compiler_params=pltpu.CompilerParams(vmem_limit_bytes=16 * MIB),
        name='attn',
    )(positions, qkv, k_cache, v_cache)

SEND_INNER = (2, 3, 1)
SEND_OUTER = (1, 2, 3)

def finish_kernel(o_ref, st_ref, hid_hbm, bo_hbm, g_hbm, b_hbm, b1_hbm, b2_hbm, wo_hbm, w1_hbm, w2_hbm, out_ref,
                  hid_ref, bo_buf, g_buf, b_buf, b1_buf, b2_buf, rows_ref, small_sem,
                  wo_buf, w1_buf, w2_buf, c1_o, c1_s, cs_o, cs_s, c2_o, c2_s, a_f32, a_bf, rs_send, rs_recv,
                  u_send, u_recv, gat, gat2, y_bf, u_bf, x_bf,
                  wo_sem, w1_sem, w2_sem, c_ssem, c_rsem, rs_ssem, rs_rsem, m_ssem, m_rsem,
                  g_ssem, g_rsem, g2_ssem, g2_rsem):
    z = lax.axis_index('tp')
    sp = lax.axis_index('sp')
    core = lax.rem(sp, 2)
    yy = sp // 2
    partner = sp + 1 - 2 * core
    across = lax.rem(sp + 2, 4)
    across_other = lax.rem(partner + 2, 4)
    zpeer = {1: z + 1 - 2 * lax.rem(z, 2), 2: lax.rem(z + 2, 4), 3: 3 - z}
    inner = (z == 0) | (z == 3)
    step = [jnp.where(inner, a, b) for a, b in zip(SEND_INNER, SEND_OUTER)]
    target = [jnp.where(inner, zpeer[a], zpeer[b]) for a, b in zip(SEND_INNER, SEND_OUTER)]
    nearest = (zpeer[1], jnp.where(inner, zpeer[3], zpeer[2]), jnp.where(inner, zpeer[2], zpeer[3]))

    smalls = [pltpu.make_async_copy(src, dst, small_sem.at[n]) for n, (src, dst) in enumerate((
        (hid_hbm, hid_ref), (bo_hbm, bo_buf), (g_hbm, g_buf), (b_hbm, b_buf), (b1_hbm, b1_buf), (b2_hbm, b2_buf)))]
    for copy in smalls:
        copy.start()
    wo_loads, w1_loads, w2_loads = [], [], []
    for j in range(4):
        cols = dyn(core * 2048 + j * 512, 512)
        wo_loads.append(pltpu.make_async_copy(wo_hbm.at[:, cols], wo_buf.at[j], wo_sem.at[j]))
        w1_loads.append(pltpu.make_async_copy(w1_hbm.at[:, cols], w1_buf.at[j], w1_sem.at[j]))
    for half, rows in enumerate((core, 1 - core)):
        for n, dest in enumerate((*target, z)):
            w2_loads.append(pltpu.make_async_copy(
                w2_hbm.at[dyn(rows * 2048, 2048), dyn(core * 2048 + dest * 512, 512)],
                w2_buf.at[half, n], w2_sem.at[half, n]))

    def begin(loads):
        for load in loads:
            load.start(priority=1)

    barrier = pltpu.get_barrier_semaphore()
    for k in (1, 2, 3):
        pl.semaphore_signal(barrier, inc=1, device_id={'tp': zpeer[k]}, device_id_type=MESH)
    for peer in (partner, across, across_other):
        pl.semaphore_signal(barrier, inc=1, device_id={'sp': peer}, device_id_type=MESH)

    pl.semaphore_wait(barrier, 6)

    def own_lanes(x):
        return jnp.where(yy == 0, x, pltpu.roll(x, 112, 1))

    c1 = (remote(st_ref, c1_s, c_ssem.at[0], c_rsem.at[0], {'sp': across}),
          remote(o_ref.at[dyn((1 - yy) * HALF_ROWS, HALF_ROWS)], c1_o, c_ssem.at[1], c_rsem.at[1], {'sp': across}))
    for copy in c1:
        copy.start()
    begin(wo_loads)
    begin(w1_loads[:1])
    for copy in smalls:
        copy.wait()
    for n, buf in enumerate((bo_buf, g_buf, b_buf, b1_buf, b2_buf)):
        rows_ref[n] = as_row(buf)
    m_a, l_a = own_lanes(st_ref[0]), own_lanes(st_ref[1])
    c1[0].wait_recv()
    m_b, l_b = own_lanes(c1_s[0]), own_lanes(c1_s[1])
    m_ab = jnp.maximum(m_a, m_b)
    f_a, f_b = jnp.exp(m_a - m_ab), jnp.exp(m_b - m_ab)
    l_ab = f_a * l_a + f_b * l_b
    cs_s[0] = m_ab
    cs_s[1] = l_ab
    c1[1].wait_recv()
    for t in range(HALF_ROWS):
        cs_o[t] = o_ref[yy * HALF_ROWS + t] * f_a[:, t:t + 1] + c1_o[t] * f_b[:, t:t + 1]

    c2 = (remote(cs_s, c2_s, c_ssem.at[2], c_rsem.at[2], {'sp': partner}),
          remote(cs_o, c2_o, c_ssem.at[3], c_rsem.at[3], {'sp': partner}))
    for copy in c2:
        copy.start()
    begin(w1_loads[1:2])
    c2[0].wait_recv()
    m_c, l_c = c2_s[0], c2_s[1]
    m_all = jnp.maximum(m_ab, m_c)
    f_ab, f_c = jnp.exp(m_ab - m_all), jnp.exp(m_c - m_all)
    inv = 1.0 / (f_ab * l_ab + f_c * l_c)
    f_ab, f_c = f_ab * inv, f_c * inv
    c2[1].wait_recv()
    for t in range(HALF_ROWS):
        a_f32[t] = cs_o[t] * f_ab[:, t:t + 1] + c2_o[t] * f_c[:, t:t + 1]
    for h in range(HEADS):
        a_bf[:, h * 128:(h + 1) * 128] = a_f32[:, h, :].astype(BF16)

    def scatter(ar, n):
        return remote(rs_send.at[ar, n], rs_recv.at[ar, step[n] - 1], rs_ssem.at[ar, n],
                      rs_rsem.at[ar, step[n] - 1], {'tp': target[n]})

    def in_plane(c, zz, n, device):
        return remote(gat.at[c, zz], gat.at[c, zz], g_ssem.at[n], g_rsem.at[c, zz], device)

    def in_group(s, zz, n, device):
        return remote(gat2.at[s, zz], gat2.at[s, zz], g2_ssem.at[n], g2_rsem.at[s, zz], device)

    my_rows = dyn(yy * HALF_ROWS, HALF_ROWS)
    my_cols = dyn(core * 2048 + z * 512, 512)

    for load in wo_loads:
        load.wait()
    pending = []
    for n in range(3):
        rs_send[0, n] = jnp.dot(a_bf[...], wo_buf[target[n]], preferred_element_type=F32)
        copy = scatter(0, n)
        copy.start()
        pending.append(copy)
    begin(w1_loads[2:])
    total = jnp.dot(a_bf[...], wo_buf[z], preferred_element_type=F32)
    resid = hid_ref[my_rows, my_cols].astype(F32) + rows_ref[0, :, my_cols] + total

    for copy in pending[:3]:
        copy.wait_recv()
    resid = (resid + (rs_recv[0, 0] + rs_recv[0, 1] + rs_recv[0, 2])).astype(BF16).astype(F32)

    gat[core, z] = resid
    sends = [in_plane(core, z, n, {'tp': target[n]}) for n in range(3)] + [in_plane(core, z, 3, {'sp': partner})]
    for copy in sends:
        copy.start()
    begin(w2_loads[:4])
    for i, peer in enumerate(nearest):
        in_plane(core, peer, 0, {'tp': peer}).wait_recv()
        copy = in_plane(core, peer, 4 + i, {'sp': partner})
        copy.start()
        sends.append(copy)
    for zz in (z, *nearest):
        in_plane(1 - core, zz, 0, {'sp': partner}).wait_recv()
    pending += sends

    begin(w2_loads[4:])
    slots = [(c, zz) for c in range(2) for zz in range(4)]
    acc = None
    for c, zz in slots:
        acc = gat[c, zz] if acc is None else acc + gat[c, zz]
    mean = jnp.sum(acc, -1, keepdims=True) * (1.0 / DIM)
    acc = None
    for c, zz in slots:
        centered = gat[c, zz] - mean
        acc = centered * centered if acc is None else acc + centered * centered
    scale = lax.rsqrt(jnp.sum(acc, -1, keepdims=True) * (1.0 / DIM) + LN_EPS)
    for c, zz in slots:
        cols = pl.ds(c * 2048 + zz * 512, 512)
        y_bf[:, cols] = ((gat[c, zz] - mean) * scale * rows_ref[1, :, cols] + rows_ref[2, :, cols]).astype(BF16)

    swaps = []
    for j in range(4):
        w1_loads[j].wait()
        part = jnp.dot(y_bf[...], w1_buf[j], preferred_element_type=F32)
        part = part + rows_ref[3, :, dyn(core * 2048 + j * 512, 512)]
        act = jnp.maximum(part, 0.0).astype(BF16)
        u_bf[:, j * 512:(j + 1) * 512] = act
        u_send[j] = act.astype(F32)
        copy = remote(u_send.at[j], u_recv.at[j], m_ssem.at[j], m_rsem.at[j], {'sp': partner})
        copy.start()
        swaps.append(copy)

    own = []
    for n in range(4):
        w2_loads[n].wait()
        own.append(jnp.dot(u_bf[...], w2_buf[0, n], preferred_element_type=F32))
    for j in range(4):
        swaps[j].wait_recv()
        x_bf[:, j * 512:(j + 1) * 512] = u_recv[j].astype(BF16)
    scatters = []
    for n in range(4):
        w2_loads[4 + n].wait()
        total = own[n] + jnp.dot(x_bf[...], w2_buf[1, n], preferred_element_type=F32)
        if n < 3:
            rs_send[1, n] = total
            copy = scatter(1, n)
            copy.start()
            scatters.append(copy)
    final = resid + rows_ref[4, :, my_cols] + total

    for copy in scatters:
        copy.wait_recv()
    final = (final + (rs_recv[1, 0] + rs_recv[1, 1] + rs_recv[1, 2])).astype(BF16).astype(F32)

    gat2[sp, z] = final
    sends = [in_group(sp, z, n, {'tp': target[n]}) for n in range(3)]
    for copy in sends:
        copy.start()

    def pass_on(slot, zz, n, peers):
        out = [in_group(slot, zz, n + i, {'sp': peer}) for i, peer in enumerate(peers)]
        for copy in out:
            copy.start()
        return out

    def hand_on(zz, n):
        in_group(across, zz, 0, {'sp': across}).wait_recv()
        return pass_on(across, zz, n, (partner,))

    sends += pass_on(sp, z, 3, (across, partner))
    for i, peer in enumerate(nearest):
        in_group(sp, peer, 0, {'tp': peer}).wait_recv()
        if i < 2:
            sends += pass_on(sp, peer, 5 + 2 * i, (across, partner))
        else:
            sends += pass_on(sp, peer, 9, (across, across_other, partner))
        if i == 1:
            sends += hand_on(z, 12)
    for i in range(2):
        sends += hand_on(nearest[i], 13 + i)
    for zz in (z, *nearest):
        in_group(partner, zz, 0, {'sp': partner}).wait_recv()
        in_group(across_other, zz, 0, {'sp': across_other}).wait_recv()
    in_group(across, nearest[2], 0, {'sp': across}).wait_recv()
    pending += sends

    for s in range(4):
        for zz in range(4):
            start = (s % 2) * 2048 + zz * 512
            out_ref[(s // 2) * 16:(s // 2) * 16 + 16, start:start + 512] = gat2[s, zz].astype(BF16)

    for copy in (*c1, *c2, *pending, *swaps, *scatters):
        copy.wait_send()

def finish_call(o_part, stats, hidden, b_out, gain, bias, b_fc1, b_fc2, w_out, w_fc1, w_fc2):
    dma = pltpu.SemaphoreType.DMA
    return pl.pallas_call(
        finish_kernel,
        out_shape=jax.ShapeDtypeStruct((ROWS, DIM), BF16),
        in_specs=[vmem_spec()] * 2 + [any_spec()] * 9,
        out_specs=vmem_spec(),
        scratch_shapes=[
            pltpu.VMEM((ROWS, DIM), BF16),
            *[pltpu.VMEM((DIM,), BF16) for _ in range(5)],
            pltpu.VMEM((5, 1, DIM), F32),
            dma((6,)),
            pltpu.VMEM((4, 1024, 512), BF16),
            pltpu.VMEM((4, DIM, 512), BF16),
            pltpu.VMEM((2, 4, 2048, 512), BF16),
            pltpu.VMEM((16, 8, 128), F32), pltpu.VMEM((2, 8, 128), F32),
            pltpu.VMEM((16, 8, 128), F32), pltpu.VMEM((2, 8, 128), F32),
            pltpu.VMEM((16, 8, 128), F32), pltpu.VMEM((2, 8, 128), F32),
            pltpu.VMEM((16, 8, 128), F32),
            pltpu.VMEM((16, 1024), BF16),
            pltpu.VMEM((2, 3, 16, 512), F32), pltpu.VMEM((2, 3, 16, 512), F32),
            pltpu.VMEM((4, 16, 512), F32), pltpu.VMEM((4, 16, 512), F32),
            pltpu.VMEM((2, 4, 16, 512), F32), pltpu.VMEM((4, 4, 16, 512), F32),
            pltpu.VMEM((16, DIM), BF16),
            pltpu.VMEM((16, 2048), BF16), pltpu.VMEM((16, 2048), BF16),
            dma((4,)), dma((4,)), dma((2, 4)), dma((4,)), dma((4,)), dma((2, 3)), dma((2, 3)),
            dma((4,)), dma((4,)), dma((7,)), dma((2, 4)), dma((15,)), dma((4, 4)),
        ],
        compiler_params=pltpu.CompilerParams(collective_id=1, has_side_effects=True, vmem_limit_bytes=48 * MIB),
        name='finish',
    )(o_part, stats, hidden, b_out, gain, bias, b_fc1, b_fc2, w_out, w_fc1, w_fc2)

def solution(mesh):
    cache_spec = P('dp', 'tp', 'sp', None)
    col_spec = P(None, 'tp')
    row_spec = P('tp', None)
    in_specs = (P('dp', None), P('dp'), cache_spec, cache_spec, P(), P(), col_spec, P('tp'), col_spec, P('tp'),
                col_spec, P('tp'), row_spec, P(), P(), P(), col_spec, P('tp'), row_spec, P())
    out_specs = (P('dp', None), cache_spec, cache_spec)

    def local_layer(hidden, positions, k_cache, v_cache, ln1_gain, ln1_bias, w_query, b_query, w_key, b_key, w_value, b_value, w_out, b_out, ln2_gain, ln2_bias, w_fc1, b_fc1, w_fc2, b_fc2):
        keep = lambda array: pltpu.with_memory_space_constraint(array, pltpu.HBM)
        qkv, k_vmem = qkv_call(*map(keep, (hidden, ln1_gain, ln1_bias, w_query, b_query, w_key, b_key, w_value, b_value, k_cache)))
        k_next, v_next, o_part, stats, _ = attn_call(keep(positions), qkv, k_vmem, keep(v_cache))
        result = finish_call(o_part, stats, *map(keep, (hidden, b_out, ln2_gain, ln2_bias, b_fc1, b_fc2, w_out, w_fc1, w_fc2)))
        return result, k_next, v_next

    return jax.shard_map(local_layer, mesh=mesh, in_specs=in_specs, out_specs=out_specs, check_vma=False)
```
